512 devices in a mesh: outer: 32 (over z_lo, y), inner: 16 (over z_hi, x, core).
Axes of the slice: x: 4, y: 8, z: 8 (z_hi: 2, z_lo: 4; z = z_hi * 4 + z_lo), core: 2. Of those that a mesh axis runs over, the one named last changes fastest.
Arguments:
- tokens: bfloat16 [4096, 4096], P('inner'), may hold values from -6 to 6
- weight_codes: int32 [2, 4096, 14336], P(None, 'inner', 'outer'), may hold values from -127 to 127
- weight_scales: float32 [2, 32, 14336], P(None, 'inner', 'outer'), may hold values from 0.000109375 to 0.0004375
- grad_codes: int32 [2, 4096, 14336], P(None, 'inner', 'outer'), may hold values from -8 to 7
- grad_scales: float32 [2, 32, 14336], P(None, 'inner', 'outer'), may hold values from 0.32 to 57.6
- cotangent: bfloat16 [4096, 14336], P('inner', 'outer'), may hold values from -6 to 6
Outputs:
- hidden: bfloat16 [4096, 14336], P('inner', 'outer')
- input_grad: bfloat16 [4096, 4096], P('inner', 'outer')
- update: float32 [2, 4096, 14336], P(None, 'inner', 'outer')
The draws below stay inside these ranges and needn't reach their ends.
All inputs are finite; a program needn't handle non-finite values.
Results may differ from the reference program's by a relative error of at most 0.023.
Values may be sent and summed in bfloat16 or wider, within the bound.
A program may use at most 128 MiB of HBM per device.

```python
import math
import jax
import jax.numpy as jnp
from jax import lax

D = 4096
FF = 14336
QBLOCK = 128
TOK_DEV = 256
TOKENS = 4096
N_OUTER = 32
N_INNER = 16


def draw_grad_scales(key, part):
    root = float(TOKENS) ** 0.5
    position = jnp.arange(FF, dtype=jnp.float32) / float(FF)
    lower = 0.01 * root
    upper = 0.05 * root
    rise = 10.0
    spread = jax.random.uniform(key, (2, D // QBLOCK, FF), jnp.float32, jnp.log(lower), jnp.log(upper))
    return jnp.exp(spread) * jnp.power(rise, position)[None, None, :]


def place_ends(result, key, smallest, largest):
    longest = result.shape.index(max(result.shape))
    spots = []
    for shift in (0, 1):
        where = [jax.random.randint(jax.random.fold_in(key, axis), (), 0, length) for axis, length in enumerate(result.shape)]
        where[longest] = (where[longest] + shift) % result.shape[longest]
        spots.append(tuple(where))
    return result.at[spots[0]].set(smallest).at[spots[1]].set(largest)


def block_scale(rng, extent, split, low, top_value):
    level = 1.0
    for axis_at, blocks in split:
        heights = jax.random.uniform(jax.random.fold_in(jax.random.fold_in(rng, 6), axis_at), (blocks,), jnp.float32, low / len(split), top_value / len(split))
        level = level * jnp.repeat(jnp.exp(heights), extent[axis_at] // blocks).reshape((-1,) + (1,) * (len(extent) - 1 - axis_at))
    return level


def bell_draw(own_key, extent, scale, limit, pieces=(), kind=jnp.bfloat16):
    result = jax.random.normal(own_key, extent, jnp.float32) * scale
    if len(pieces) > 0:
        result = block_scale(own_key, extent, pieces, -0.22, 0.18) * result
    return jnp.clip(result, min=-limit, max=limit).astype(kind)


def setup_inputs(seed: int = 0) -> dict:
    key_list = jax.random.split(jax.random.key(seed), 7)
    tokens = bell_draw(key_list[0], (TOKENS, D), 1.0, 6.0, ((0, 16),))
    weight_codes = place_ends(jax.random.randint(key_list[1], (2, D, FF), -127, 128), jax.random.fold_in(key_list[1], 1), -127, 127).astype(jnp.int32)
    weight_scales = jnp.clip(jnp.exp(math.log(0.0004375) - 1.3862944 * jax.random.uniform(key_list[2], (2, D // QBLOCK, FF), jnp.float32) ** block_scale(key_list[2], (2, D // QBLOCK, FF), ((1, 16), (2, 32)), -0.2, 0.2)), 0.000109375, 0.0004375)
    grad_codes = place_ends(jax.random.randint(key_list[3], (2, D, FF), -8, 8), jax.random.fold_in(key_list[3], 1), -8, 7).astype(jnp.int32)
    grad_scales = draw_grad_scales(jax.random.fold_in(key_list[6], 71), 0)
    cotangent = bell_draw(key_list[5], (TOKENS, FF), 1.0, 6.0, ((0, 16), (1, 32)))
    return {"tokens": tokens, "weight_codes": weight_codes, "weight_scales": weight_scales, "grad_codes": grad_codes, "grad_scales": grad_scales, "cotangent": cotangent}


def dequantize(codes, scales):
    count, rows, cols = codes.shape
    blocks = codes.reshape(count, rows // QBLOCK, QBLOCK, cols).astype(jnp.float32) * scales[:, :, None, :]
    return blocks.reshape(count, rows, cols)

def reference(tokens, weight_codes, weight_scales, grad_codes, grad_scales, cotangent):
    weights = dequantize(weight_codes, weight_scales).astype(jnp.bfloat16)
    gate = jnp.dot(tokens, weights[0], preferred_element_type=jnp.float32)
    up = jnp.dot(tokens, weights[1], preferred_element_type=jnp.float32)
    sig = jax.nn.sigmoid(gate)
    hidden = (gate * sig * up).astype(jnp.bfloat16)
    back = cotangent.astype(jnp.float32)
    d_gate = (back * up * sig * (1.0 + gate * (1.0 - sig))).astype(jnp.bfloat16)
    d_up = (back * gate * sig).astype(jnp.bfloat16)
    width = FF // N_OUTER

    def input_step(total, index):
        start = (index * width).astype(jnp.int32)
        piece_g = lax.dynamic_slice_in_dim(d_gate, start, width, 1)
        piece_u = lax.dynamic_slice_in_dim(d_up, start, width, 1)
        rows_g = lax.dynamic_slice_in_dim(weights[0], start, width, 1)
        rows_u = lax.dynamic_slice_in_dim(weights[1], start, width, 1)
        part = jnp.dot(piece_g, rows_g.T, preferred_element_type=jnp.float32)
        part = part + jnp.dot(piece_u, rows_u.T, preferred_element_type=jnp.float32)
        rounded = lax.optimization_barrier(part.astype(jnp.bfloat16))
        return (total + rounded.astype(jnp.float32), None)
    input_total, unused = lax.scan(input_step, jnp.zeros((TOKENS, D), jnp.float32), jnp.arange(N_OUTER, dtype=jnp.int32))

    def grad_step(total, index):
        start = (index * TOK_DEV).astype(jnp.int32)
        block_x = lax.dynamic_slice_in_dim(tokens, start, TOK_DEV, 0)
        block_g = lax.dynamic_slice_in_dim(d_gate, start, TOK_DEV, 0)
        block_u = lax.dynamic_slice_in_dim(d_up, start, TOK_DEV, 0)
        part_g = lax.optimization_barrier(jnp.dot(block_x.T, block_g, preferred_element_type=jnp.float32).astype(jnp.bfloat16))
        part_u = lax.optimization_barrier(jnp.dot(block_x.T, block_u, preferred_element_type=jnp.float32).astype(jnp.bfloat16))
        both = jnp.stack([part_g.astype(jnp.float32), part_u.astype(jnp.float32)])
        return (total + both, None)
    grads, unused = lax.scan(grad_step, jnp.zeros((2, D, FF), jnp.float32), jnp.arange(N_INNER, dtype=jnp.int32))
    total = dequantize(grad_codes, grad_scales) + grads
    rms = jnp.sqrt(jnp.sum(total * total) / (2.0 * D * FF) + 1e-06)
    update = total / rms
    return (hidden, input_total.astype(jnp.bfloat16), update)
```

```python
import functools

import jax
import jax.numpy as jnp
from jax import lax
from jax.experimental import pallas as pl
from jax.experimental.pallas import tpu as pltpu
from jax.sharding import Mesh
from jax.sharding import PartitionSpec as P

D = 4096
FF = 14336
QBLOCK = 128
INNER = ("inner_0", "inner_1", "inner_2")
OUTER = ("outer_0", "outer_1")
ROWS = 256
COLS = 448
CAT = 2 * COLS
MESH = pl.DeviceIdType.MESH
F32 = jnp.float32
BF16 = jnp.bfloat16

PAIRS = ((0, 2, 0), (1, 3, 1), (4, 5, 2))
MIXED = 6

GATHER_SLOTS = {
    name: k
    for k, name in enumerate(
        [f"{b}{h}" for b in ("l", "r", "a") for h in range(2)]
        + [f"{b}{q}" for b in ("p", "pl", "pr", "pa") for q in range(4)]
    )
}
ROLES = ("own", "r", "l", "a", "p", "pr", "pl", "pa")


def tile(t):
    return slice(t * 128, (t + 1) * 128)


def wait_bytes(ref, sem):
    pltpu.make_async_copy(ref, ref, sem).wait()


class Gather:
    def __init__(self, at, buf, transit, send, recv, relay, sib):
        self.at, self.buf, self.transit = at, buf, transit
        self.send, self.recv, self.relay, self.sib = send, recv, relay, sib
        zh, x, c = at["zh"], at["x"], at["c"]

        def chip(h, k):
            return h * 4 + lax.rem(x + k, 4)

        other = 1 - zh
        self.chip = {
            "own": chip(zh, 0),
            "r": chip(zh, 1),
            "a": chip(zh, 2),
            "l": chip(zh, 3),
            "p": chip(other, 0),
            "pr": chip(other, 1),
            "pa": chip(other, 2),
            "pl": chip(other, 3),
        }

    def rows(self, role, first, count, sibling=False):
        c = self.at["c"]
        block = self.chip[role] * 2 + (1 - c if sibling else c)
        return self.buf.at[pl.ds(pl.multiple_of(block * ROWS + first, 64), count)]

    def copy(self, src, dst, recv, where):
        pltpu.make_async_remote_copy(
            src_ref=src,
            dst_ref=dst,
            send_sem=self.send,
            recv_sem=recv,
            device_id=where,
            device_id_type=MESH,
        ).start()

    def along_x(self, role, first, count, right, slot):
        part = self.rows(role, first, count)
        where = {"inner_1": self.at["right"] if right else self.at["left"]}
        self.copy(part, part, self.recv.at[GATHER_SLOTS[slot]], where)

    def along_z(self, q):
        part = self.rows("own", q * 64, 64)
        where = self.at["up2"] if q < 2 else self.at["down2"]
        self.copy(part, self.transit.at[q], self.relay.at[q], where)

    def pass_on(self, q):
        wait_bytes(self.transit.at[q], self.relay.at[q])
        at = self.at
        origin = at["down2"] if q < 2 else at["up2"]
        where = at["up2"] if q < 2 else at["down2"]
        block = (origin["inner_0"] * 4 + at["x"]) * 2 + at["c"]
        dst = self.buf.at[pl.ds(pl.multiple_of(block * ROWS + q * 64, 64), 64)]
        self.copy(self.transit.at[q], dst, self.recv.at[GATHER_SLOTS[f"p{q}"]], where)

    def to_sibling(self, role):
        part = self.rows(role, 0, ROWS)
        self.copy(part, part, self.sib.at[ROLES.index(role)], {"inner_2": 1 - self.at["c"]})

    def start(self):
        for q in (0, 2):
            self.along_z(q)
        self.along_x("own", 0, 128, True, "l0")
        self.along_x("own", 128, 128, False, "r1")
        for q in (1, 3):
            self.along_z(q)
        self.along_x("own", 128, 128, True, "l1")
        self.along_x("own", 0, 128, False, "r0")
        self.to_sibling("own")

    def wait_half(self, role, h):
        wait_bytes(self.rows(role, h * 128, 128), self.recv.at[GATHER_SLOTS[f"{role}{h}"]])

    def wait_quarter(self, role, q):
        wait_bytes(self.rows(role, q * 64, 64), self.recv.at[GATHER_SLOTS[f"{role}{q}"]])

    def first_hop(self):
        self.wait_half("l", 0)
        self.along_x("l", 0, 128, True, "a0")
        self.wait_half("r", 1)
        self.along_x("r", 128, 128, False, "a1")

    def near_done(self):
        self.wait_half("l", 1)
        self.to_sibling("l")
        self.wait_half("r", 0)
        self.to_sibling("r")

    def far_done(self):
        self.wait_half("a", 0)
        self.wait_half("a", 1)
        self.to_sibling("a")

    def partner(self, qs):
        for q in qs:
            self.wait_quarter("p", q)
            self.along_x("p", q * 64, 64, True, f"pl{q}")
            self.along_x("p", q * 64, 64, False, f"pr{q}")

    def partner_hop(self, up, down):
        self.wait_quarter("pl", up)
        self.along_x("pl", up * 64, 64, True, f"pa{up}")
        self.wait_quarter("pr", down)
        self.along_x("pr", down * 64, 64, False, f"pa{down}")

    def partner_near_done(self):
        for q in (2, 3):
            self.wait_quarter("pl", q)
        self.to_sibling("pl")
        for q in (0, 1):
            self.wait_quarter("pr", q)
        self.to_sibling("pr")

    def partner_far_done(self):
        for q in (0, 2, 1, 3):
            self.wait_quarter("pa", q)
        self.to_sibling("pa")

    def unit(self, role):
        wait_bytes(self.rows(role, 0, ROWS, True), self.sib.at[ROLES.index(role)])
        return pl.multiple_of(self.chip[role] * 512, 512)

    def finish(self):
        wait_bytes(self.buf, self.send)


def kernel(
    tok_h,
    wc_h,
    ws_h,
    gc_h,
    gs_h,
    cot_h,
    hid_o,
    ig_o,
    upd_o,
    tok,
    wc,
    ws,
    gc,
    gs,
    cot,
    wbuf,
    dbuf,
    wtransit,
    dtransit,
    xt,
    acc,
    term,
    landed,
    zsend,
    zland,
    igacc,
    hid,
    ig,
    upd,
    part,
    parts,
    load_sem,
    out_sem,
    wsend,
    wrecv,
    wrelay,
    wsib,
    dsend,
    drecv,
    drelay,
    dsib,
    xsend,
    xrecv,
    ysend,
    yrecv,
    rsend,
    rrecv,
    zs_send,
    zs_recv,
    msend,
    mrecv,
):
    zl, y = lax.axis_index("outer_0"), lax.axis_index("outer_1")
    zh, x, c = (lax.axis_index(a) for a in INNER)
    z = zh * 4 + zl
    me = (zh * 4 + x) * 2 + c

    def z_at(k):
        there = lax.rem(z + k, 8)
        return {"outer_0": lax.rem(there, 4), "inner_0": there // 4}

    def inner_at(k):
        there = lax.rem(me + k, 16)
        return there, {
            "inner_0": there // 8,
            "inner_1": lax.rem(there // 2, 4),
            "inner_2": lax.rem(there, 2),
        }

    def plane_at(k):
        there = lax.rem(x * 2 + c + k, 8)
        return {"inner_1": there // 2, "inner_2": lax.rem(there, 2)}

    def y_at(k):
        return {"outer_1": lax.rem(y + k, 8)}

    at = {
        "zh": zh,
        "x": x,
        "c": c,
        "right": lax.rem(x + 1, 4),
        "left": lax.rem(x + 3, 4),
        "up2": z_at(2),
        "down2": z_at(6),
    }

    barrier = pltpu.get_barrier_semaphore()
    greeted = [inner_at(k)[1] for k in range(1, 16)]
    greeted += [z_at(k) for k in (1, 2, 3, 5, 6, 7)]
    greeted += [y_at(k) for k in range(1, 8)]
    for where in greeted:
        pl.semaphore_signal(barrier, inc=1, device_id=where, device_id_type=MESH)

    loads = [
        pltpu.make_async_copy(src, dst, load_sem.at[k])
        for k, (src, dst) in enumerate(
            ((ws_h, ws), (wc_h, wc), (tok_h, tok), (cot_h, cot), (gs_h, gs), (gc_h, gc))
        )
    ]
    for load in loads:
        load.start()

    loads[0].wait()
    loads[1].wait()
    own_row = pl.multiple_of(me * ROWS, ROWS)

    def dequantize(i, carry, half):
        here = pl.ds(pl.multiple_of(half * QBLOCK + i * 32, 32), 32)
        there = pl.ds(pl.multiple_of(own_row + half * QBLOCK + i * 32, 32), 32)

        def value(k, lanes):
            return wc[k, here, lanes].astype(F32) * ws[k, half : half + 1, lanes]

        for g, u, t in PAIRS:
            wbuf[there, tile(g)] = value(0, tile(t)).astype(BF16)
            wbuf[there, tile(u)] = value(1, tile(t)).astype(BF16)
        last = slice(384, 448)
        mixed = jnp.concatenate([value(0, last), value(1, last)], axis=1)
        wbuf[there, tile(MIXED)] = mixed.astype(BF16)
        return carry

    for half in range(2):
        lax.fori_loop(0, QBLOCK // 32, functools.partial(dequantize, half=half), 0)
    loads[2].wait()
    pl.semaphore_wait(barrier, len(greeted))

    own_tokens = pl.ds(pl.multiple_of(y * 32, 32), 32)
    for k in range(1, 16):
        there, where = inner_at(k)
        pltpu.make_async_remote_copy(
            src_ref=tok.at[own_tokens, pl.ds(pl.multiple_of(there * ROWS, ROWS), ROWS)],
            dst_ref=xt.at[me, y],
            send_sem=xsend,
            recv_sem=xrecv,
            device_id=where,
            device_id_type=MESH,
        ).start()
    weights = Gather(at, wbuf, wtransit, wsend, wrecv, wrelay, wsib)
    weights.start()
    xt[me, y] = tok[own_tokens, pl.ds(pl.multiple_of(me * ROWS, ROWS), ROWS)]

    def y_share(k, right, slot):
        share = xt.at[:, lax.rem(y + k, 8)]
        pltpu.make_async_remote_copy(
            src_ref=share,
            dst_ref=share,
            send_sem=ysend,
            recv_sem=yrecv.at[slot],
            device_id=y_at(1 if right else 7),
            device_id_type=MESH,
        ).start()

    def y_wait(k, slot):
        wait_bytes(xt.at[:, lax.rem(y + k, 8)], yrecv.at[slot])

    def y_first():
        wait_bytes(xt.at[pl.ds(0, 15), 0], xrecv)
        y_share(0, True, 0)
        y_share(0, False, 4)

    def y_step(s):
        y_wait(8 - s, s - 1)
        if s < 4:
            y_share(8 - s, True, s)
        if s < 4:
            y_wait(s, 3 + s)
        if s < 3:
            y_share(s, False, 4 + s)

    def multiply(role, first=False):
        row = weights.unit(role)
        product = jnp.dot(
            tok[:, pl.ds(row, 512)], wbuf[pl.ds(row, 512), :], preferred_element_type=F32
        )
        acc[...] = product if first else acc[...] + product

    multiply("own", True)
    y_first()
    weights.first_hop()
    for q in (0, 2):
        weights.pass_on(q)
    weights.near_done()
    y_step(1)
    for q in (1, 3):
        weights.pass_on(q)
    weights.partner((0, 2))
    multiply("r")
    multiply("l")
    weights.far_done()
    y_step(2)
    multiply("a")
    weights.partner_hop(0, 2)
    weights.partner((1, 3))
    weights.to_sibling("p")
    weights.partner_hop(1, 3)
    weights.partner_near_done()
    y_step(3)
    multiply("p")
    weights.partner_far_done()
    multiply("pl")
    multiply("pr")
    multiply("pa")

    loads[3].wait()

    def activate(i, carry):
        here = pl.ds(pl.multiple_of(i * 32, 32), 32)
        there = pl.ds(pl.multiple_of(own_row + i * 32, 32), 32)

        def grads(gate, up, back):
            sig = jax.nn.sigmoid(gate)
            d_gate = back * up * sig * (1.0 + gate * (1.0 - sig))
            return gate * sig * up, d_gate, back * gate * sig

        for g, u, t in PAIRS:
            back = cot[here, tile(t)].astype(F32)
            value, d_gate, d_up = grads(acc[here, tile(g)], acc[here, tile(u)], back)
            hid[here, tile(t)] = value.astype(BF16)
            dbuf[there, tile(g)] = d_gate.astype(BF16)
            dbuf[there, tile(u)] = d_up.astype(BF16)
        last = slice(384, 448)
        mixed = acc[here, tile(MIXED)]
        back = cot[here, last].astype(F32)
        gate, up = mixed[:, :64], pltpu.roll(mixed, 64, 1)[:, :64]
        value, d_gate, d_up = grads(gate, up, back)
        hid[here, last] = value.astype(BF16)
        dbuf[there, tile(MIXED)] = jnp.concatenate([d_gate, d_up], axis=1).astype(BF16)
        return carry

    lax.fori_loop(0, ROWS // 32, activate, 0)

    deltas = Gather(at, dbuf, dtransit, dsend, drecv, drelay, dsib)
    deltas.start()
    hid_out = pltpu.make_async_copy(hid, hid_o, out_sem.at[0])
    hid_out.start()

    def partial_inputs(k):
        pair = lax.rem(lax.rem(y + 4, 8) // 2 + k, 4)
        own = dbuf[pl.ds(own_row, ROWS), :]
        for run in range(4):
            row = pl.multiple_of((run * 4 + pair) * ROWS, ROWS)
            product = lax.dot_general(
                own,
                wbuf[pl.ds(row, ROWS), :],
                (((1,), (1,)), ((), ())),
                preferred_element_type=F32,
            ).astype(BF16)
            term[pair * 2, run] = product[:, :128]
            term[pair * 2 + 1, run] = product[:, 128:]

    def target(d, s):
        return lax.rem(y + (4 - s if d == 0 else 4 + s), 8)

    def reduce_send(d, s, h):
        pltpu.make_async_remote_copy(
            src_ref=term.at[target(d, s), pl.ds(h * 2, 2)],
            dst_ref=landed.at[d, s, h],
            send_sem=rsend,
            recv_sem=rrecv.at[(d * 4 + s) * 2 + h],
            device_id=y_at(1 if d == 0 else 7),
            device_id_type=MESH,
        ).start()

    def reduce_wait(d, s, h):
        wait_bytes(landed.at[d, s, h], rrecv.at[(d * 4 + s) * 2 + h])

    def reduce_step(d, s, h):
        reduce_wait(d, s, h)
        goal = target(d, s + 1)

        def add(i, carry):
            here = pl.ds(pl.multiple_of(i * 64, 64), 64)
            for k in range(2):
                came = landed[d, s, h, k, here].astype(F32)
                mine = term[goal, h * 2 + k, here].astype(F32)
                term[goal, h * 2 + k, here] = (mine + came).astype(BF16)
            return carry

        lax.fori_loop(0, ROWS // 64, add, 0)
        reduce_send(d, s + 1, h)

    def reduce_last():
        for h in range(2):
            for d in range(2):
                reduce_wait(d, 3, h)
        for k in (1, 2, 3, 0):
            run = lax.rem(zl + k, 4)

            def add(i, carry, k=k, run=run):
                here = pl.ds(pl.multiple_of(i * 64, 64), 64)
                total = term[y, run, here].astype(F32)
                for d in range(2):
                    total = total + landed[d, 3, run // 2, lax.rem(run, 2), here].astype(F32)
                if k:
                    zsend[k - 1, here] = total.astype(BF16)
                else:
                    igacc[here] = total
                return carry

            lax.fori_loop(0, ROWS // 64, add, 0)
            if k:
                pltpu.make_async_remote_copy(
                    src_ref=zsend.at[k - 1],
                    dst_ref=zland.at[k - 1],
                    send_sem=zs_send,
                    recv_sem=zs_recv,
                    device_id={"outer_0": run},
                    device_id_type=MESH,
                ).start()

    def input_done():
        wait_bytes(zland, zs_recv)

        def add(i, carry):
            here = pl.ds(pl.multiple_of(i * 64, 64), 64)
            total = igacc[here]
            for k in range(3):
                total = total + zland[k, here].astype(F32)
            ig[here] = total.astype(BF16)
            return carry

        lax.fori_loop(0, ROWS // 64, add, 0)

    def accumulate(role, first=False):
        row = deltas.unit(role)
        block = xt[pl.ds(pl.multiple_of(deltas.chip[role] * 2, 2), 2)].reshape(512, ROWS)
        product = lax.dot_general(
            block,
            dbuf[pl.ds(row, 512), :],
            (((0,), (0,)), ((), ())),
            preferred_element_type=F32,
        )
        acc[...] = product if first else acc[...] + product

    partial_inputs(0)
    reduce_send(0, 0, 0)
    reduce_send(1, 0, 1)
    partial_inputs(1)
    partial_inputs(3)
    reduce_send(0, 1, 1)
    reduce_send(1, 1, 0)
    partial_inputs(2)
    y_step(4)
    accumulate("own", True)
    deltas.first_hop()
    reduce_step(0, 0, 0)
    reduce_step(1, 0, 1)
    for q in (0, 2):
        deltas.pass_on(q)
    reduce_step(0, 1, 1)
    reduce_step(1, 1, 0)
    deltas.near_done()
    reduce_step(0, 1, 0)
    reduce_step(1, 1, 1)
    for q in (1, 3):
        deltas.pass_on(q)
    deltas.partner((0, 2))
    reduce_step(0, 2, 1)
    reduce_step(1, 2, 0)
    accumulate("r")
    accumulate("l")
    deltas.far_done()
    reduce_step(0, 2, 0)
    reduce_step(1, 2, 1)
    deltas.partner_hop(0, 2)
    deltas.partner((1, 3))
    deltas.to_sibling("p")
    reduce_last()
    accumulate("a")
    deltas.partner_hop(1, 3)
    deltas.partner_near_done()
    accumulate("p")
    input_done()
    ig_out = pltpu.make_async_copy(ig, ig_o, out_sem.at[1])
    ig_out.start()
    deltas.partner_far_done()
    accumulate("pl")
    accumulate("pr")
    accumulate("pa")

    loads[4].wait()
    loads[5].wait()

    def totals(i, carry, half):
        wide, narrow = carry
        here = pl.ds(pl.multiple_of(half * QBLOCK + i * 32, 32), 32)

        def add(k, lanes, grad):
            total = gc[k, here, lanes].astype(F32) * gs[k, half : half + 1, lanes] + grad
            upd[k, here, lanes] = total
            return jnp.sum((total * total).reshape(4, 8, total.shape[1]), axis=0)

        for g, u, t in PAIRS:
            wide = wide + add(0, tile(t), acc[here, tile(g)])
            wide = wide + add(1, tile(t), acc[here, tile(u)])
        last = slice(384, 448)
        mixed = acc[here, tile(MIXED)]
        narrow = narrow + add(0, last, mixed[:, :64])
        narrow = narrow + add(1, last, pltpu.roll(mixed, 64, 1)[:, :64])
        return wide, narrow

    squares = (jnp.zeros((8, 128), F32), jnp.zeros((8, 64), F32))
    for half in range(2):
        squares = lax.fori_loop(0, QBLOCK // 32, functools.partial(totals, half=half), squares)
    wide, narrow = squares
    part[0] = jnp.broadcast_to(
        jnp.sum(wide, keepdims=True) + jnp.sum(narrow, keepdims=True), (8, 128)
    )
    value = part[0]
    for stage, peer in enumerate((plane_at, z_at, y_at)):
        for k in range(1, 8):
            pltpu.make_async_remote_copy(
                src_ref=part.at[stage],
                dst_ref=parts.at[stage, k - 1],
                send_sem=msend.at[stage],
                recv_sem=mrecv.at[stage],
                device_id=peer(k),
                device_id_type=MESH,
            ).start()
        wait_bytes(parts.at[stage], mrecv.at[stage])
        for k in range(7):
            value = value + parts[stage, k]
        if stage < 2:
            part[stage + 1] = value
    scale = 1.0 / jnp.sqrt(value / (2.0 * D * FF) + 1e-06)
    scale = scale[0:1, 0:1]

    outs = []
    for half in range(2):

        def normalize(i, carry, half=half):
            here = pl.ds(pl.multiple_of(half * 128 + i * 32, 32), 32)
            for k in range(2):
                upd[k, here, :] = upd[k, here, :] * scale
            return carry

        lax.fori_loop(0, 4, normalize, 0)
        rows = pl.ds(half * 128, 128)
        out = pltpu.make_async_copy(upd.at[:, rows], upd_o.at[:, rows], out_sem.at[2 + half])
        out.start()
        outs.append(out)

    weights.finish()
    deltas.finish()
    wait_bytes(xt.at[pl.ds(0, 15), 0], xsend)
    wait_bytes(xt.at[:, pl.ds(0, 7)], ysend)
    wait_bytes(term.at[pl.ds(0, 7)], rsend)
    wait_bytes(zsend, zs_send)
    for stage in range(3):
        wait_bytes(parts.at[stage], msend.at[stage])
    hid_out.wait()
    ig_out.wait()
    for out in outs:
        out.wait()


def local(tokens, weight_codes, weight_scales, grad_codes, grad_scales, cotangent):
    dma = pltpu.SemaphoreType.DMA
    slots = len(GATHER_SLOTS)
    gather = [dma, dma((slots,)), dma((4,)), dma((8,))]
    call = pl.pallas_call(
        kernel,
        out_shape=(
            jax.ShapeDtypeStruct((ROWS, COLS), BF16),
            jax.ShapeDtypeStruct((ROWS, 128), BF16),
            jax.ShapeDtypeStruct((2, ROWS, COLS), F32),
        ),
        in_specs=[pl.BlockSpec(memory_space=pl.ANY)] * 6,
        out_specs=[pl.BlockSpec(memory_space=pl.ANY)] * 3,
        scratch_shapes=[
            pltpu.VMEM((ROWS, D), BF16),
            pltpu.VMEM((2, ROWS, COLS), jnp.int32),
            pltpu.VMEM((2, 2, COLS), F32),
            pltpu.VMEM((2, ROWS, COLS), jnp.int32),
            pltpu.VMEM((2, 2, COLS), F32),
            pltpu.VMEM((ROWS, COLS), BF16),
            pltpu.VMEM((16 * ROWS, CAT), BF16),
            pltpu.VMEM((16 * ROWS, CAT), BF16),
            pltpu.VMEM((4, 64, CAT), BF16),
            pltpu.VMEM((4, 64, CAT), BF16),
            pltpu.VMEM((16, 8, 32, ROWS), BF16),
            pltpu.VMEM((ROWS, CAT), F32),
            pltpu.VMEM((8, 4, ROWS, 128), BF16),
            pltpu.VMEM((2, 4, 2, 2, ROWS, 128), BF16),
            pltpu.VMEM((3, ROWS, 128), BF16),
            pltpu.VMEM((3, ROWS, 128), BF16),
            pltpu.VMEM((ROWS, 128), F32),
            pltpu.VMEM((ROWS, COLS), BF16),
            pltpu.VMEM((ROWS, 128), BF16),
            pltpu.VMEM((2, ROWS, COLS), F32),
            pltpu.VMEM((3, 8, 128), F32),
            pltpu.VMEM((3, 7, 8, 128), F32),
            dma((6,)),
            dma((4,)),
            *gather,
            *gather,
            dma,
            dma,
            dma,
            dma((7,)),
            dma,
            dma((16,)),
            dma,
            dma,
            dma((3,)),
            dma((3,)),
        ],
        compiler_params=pltpu.CompilerParams(
            collective_id=0, has_side_effects=True, vmem_limit_bytes=60 * 1024 * 1024
        ),
    )
    return tuple(
        call(tokens, weight_codes, weight_scales, grad_codes, grad_scales, cotangent)
    )


def solution(mesh):
    finer = Mesh(
        mesh.devices.reshape(4, 8, 2, 4, 2), ("outer_0", "outer_1", "inner_0", "inner_1", "inner_2")
    )
    return jax.shard_map(
        local,
        mesh=finer,
        in_specs=(
            P(INNER, None),
            P(None, INNER, OUTER),
            P(None, INNER, OUTER),
            P(None, INNER, OUTER),
            P(None, INNER, OUTER),
            P(INNER, OUTER),
        ),
        out_specs=(P(INNER, OUTER), P(INNER, OUTER), P(None, INNER, OUTER)),
        check_vma=False,
    )
```

```python
import jax
import jax.numpy as jnp
from jax import lax
from jax.experimental import pallas as pl
from jax.experimental.pallas import tpu as pltpu
from jax.sharding import Mesh
from jax.sharding import PartitionSpec as P

D = 4096
FF = 14336
QBLOCK = 128
INNER = ("inner_0", "inner_1", "inner_2")
OUTER = ("outer_0", "outer_1")
ROWS = 256
COLS = 448
CAT = 2 * COLS
MESH = pl.DeviceIdType.MESH
F32 = jnp.float32
BF16 = jnp.bfloat16

HALF = COLS
PIECE = COLS // 4

GATHER_SLOTS = {
    name: k
    for k, name in enumerate(
        [f"{b}{h}" for b in ("l", "r", "a") for h in range(2)]
        + [f"{b}{q}" for b in ("p", "pl", "pr", "pa") for q in range(8)]
    )
}
ROLES = ("own", "r", "l", "a", "p", "pr", "pl", "pa")


def wait_bytes(ref, sem):
    pltpu.make_async_copy(ref, ref, sem).wait()


class Gather:
    def __init__(self, at, buf, transit, send, recv, relay, sib):
        self.at, self.buf, self.transit = at, buf, transit
        self.send, self.recv, self.relay, self.sib = send, recv, relay, sib
        zh, x, c = at["zh"], at["x"], at["c"]

        def chip(h, k):
            return h * 4 + lax.rem(x + k, 4)

        other = 1 - zh
        self.chip = {
            "own": chip(zh, 0),
            "r": chip(zh, 1),
            "a": chip(zh, 2),
            "l": chip(zh, 3),
            "p": chip(other, 0),
            "pr": chip(other, 1),
            "pa": chip(other, 2),
            "pl": chip(other, 3),
        }

    def rows(self, role, first, count, sibling=False):
        c = self.at["c"]
        block = self.chip[role] * 2 + (1 - c if sibling else c)
        return self.buf.at[pl.ds(pl.multiple_of(block * CAT + first, 16), count)]

    def piece(self, role, q):
        return self.rows(role, q * PIECE, PIECE)

    def copy(self, src, dst, recv, where):
        pltpu.make_async_remote_copy(
            src_ref=src,
            dst_ref=dst,
            send_sem=self.send,
            recv_sem=recv,
            device_id=where,
            device_id_type=MESH,
        ).start()

    def along_x(self, part, right, slot):
        where = {"inner_1": self.at["right"] if right else self.at["left"]}
        self.copy(part, part, self.recv.at[GATHER_SLOTS[slot]], where)

    def half(self, role, h):
        return self.rows(role, h * HALF, HALF)

    def along_z(self, q):
        where = self.at["up2"] if q < 4 else self.at["down2"]
        self.copy(self.piece("own", q), self.transit.at[q], self.relay.at[q], where)

    def pass_on(self, k):
        at = self.at
        for q in (k, k + 4):
            wait_bytes(self.transit.at[q], self.relay.at[q])
            origin = at["down2"] if q < 4 else at["up2"]
            where = at["up2"] if q < 4 else at["down2"]
            block = (origin["inner_0"] * 4 + at["x"]) * 2 + at["c"]
            dst = self.buf.at[pl.ds(pl.multiple_of(block * CAT + q * PIECE, 16), PIECE)]
            self.copy(self.transit.at[q], dst, self.recv.at[GATHER_SLOTS[f"p{q}"]], where)

    def to_sibling(self, role):
        part = self.rows(role, 0, CAT)
        self.copy(part, part, self.sib.at[ROLES.index(role)], {"inner_2": 1 - self.at["c"]})

    def start_z(self, ks):
        for k in ks:
            self.along_z(k)
            self.along_z(k + 4)

    def start_x(self):
        self.along_x(self.half("own", 0), True, "l0")
        self.along_x(self.half("own", 1), False, "r1")
        self.along_x(self.half("own", 1), True, "l1")
        self.along_x(self.half("own", 0), False, "r0")
        self.to_sibling("own")

    def wait_half(self, role, h):
        wait_bytes(self.half(role, h), self.recv.at[GATHER_SLOTS[f"{role}{h}"]])

    def wait_piece(self, role, q):
        wait_bytes(self.piece(role, q), self.recv.at[GATHER_SLOTS[f"{role}{q}"]])

    def first_hop(self):
        self.wait_half("l", 0)
        self.along_x(self.half("l", 0), True, "a0")
        self.wait_half("r", 1)
        self.along_x(self.half("r", 1), False, "a1")

    def near_done(self):
        self.wait_half("l", 1)
        self.to_sibling("l")
        self.wait_half("r", 0)
        self.to_sibling("r")

    def far_done(self):
        self.wait_half("a", 0)
        self.wait_half("a", 1)
        self.to_sibling("a")

    def partner(self, k):
        for q in (k, k + 4):
            self.wait_piece("p", q)
            self.along_x(self.piece("p", q), True, f"pl{q}")
            self.along_x(self.piece("p", q), False, f"pr{q}")
        if k == 3:
            self.to_sibling("p")

    def partner_hop(self, k):
        self.wait_piece("pl", k)
        self.along_x(self.piece("pl", k), True, f"pa{k}")
        self.wait_piece("pr", k + 4)
        self.along_x(self.piece("pr", k + 4), False, f"pa{k + 4}")

    def partner_near_done(self):
        for q in range(4, 8):
            self.wait_piece("pl", q)
        self.to_sibling("pl")
        for q in range(4):
            self.wait_piece("pr", q)
        self.to_sibling("pr")

    def partner_far_done(self):
        for k in range(4):
            self.wait_piece("pa", k)
            self.wait_piece("pa", k + 4)
        self.to_sibling("pa")

    def blocks(self, role):
        c = self.at["c"]
        for k, which in enumerate((c, 1 - c)):
            if k:
                wait_bytes(self.rows(role, 0, CAT, True), self.sib.at[ROLES.index(role)])
            number = self.chip[role] * 2 + which
            yield number, self.block(number)

    def block(self, number):
        return self.buf[pl.ds(pl.multiple_of(number * CAT, CAT), CAT), :]

    def finish(self):
        wait_bytes(self.buf, self.send)


def kernel(
    tok_h,
    wc_h,
    ws_h,
    gc_h,
    gs_h,
    cot_h,
    hid,
    ig,
    upd,
    scale,
    tok,
    wc,
    ws,
    gc,
    gs,
    cot,
    wbuf,
    dbuf,
    wtransit,
    dtransit,
    xt,
    acc,
    term,
    landed,
    zsend,
    zland,
    igacc,
    own,
    lanes,
    column,
    part,
    parts,
    load_sem,
    wsend,
    wrecv,
    wrelay,
    wsib,
    dsend,
    drecv,
    drelay,
    dsib,
    xsend,
    xrecv,
    ysend,
    yrecv,
    rsend,
    rrecv,
    zs_send,
    zs_recv,
    msend,
    mrecv,
):
    zl, y = lax.axis_index("outer_0"), lax.axis_index("outer_1")
    zh, x, c = (lax.axis_index(a) for a in INNER)
    z = zh * 4 + zl
    me = (zh * 4 + x) * 2 + c

    def z_at(k):
        there = lax.rem(z + k, 8)
        return {"outer_0": lax.rem(there, 4), "inner_0": there // 4}

    def inner_at(k):
        there = lax.rem(me + k, 16)
        return there, {
            "inner_0": there // 8,
            "inner_1": lax.rem(there // 2, 4),
            "inner_2": lax.rem(there, 2),
        }

    def plane_at(k):
        there = lax.rem(x * 2 + c + k, 8)
        return {"inner_1": there // 2, "inner_2": lax.rem(there, 2)}

    def y_at(k):
        return {"outer_1": lax.rem(y + k, 8)}

    at = {
        "zh": zh,
        "x": x,
        "c": c,
        "right": lax.rem(x + 1, 4),
        "left": lax.rem(x + 3, 4),
        "up2": z_at(2),
        "down2": z_at(6),
    }

    loads = [
        pltpu.make_async_copy(src, dst, load_sem.at[k])
        for k, (src, dst) in enumerate(
            ((ws_h, ws), (wc_h, wc), (tok_h, tok), (cot_h, cot), (gs_h, gs), (gc_h, gc))
        )
    ]
    for load in loads:
        load.start()

    barrier = pltpu.get_barrier_semaphore()
    greeted = [inner_at(k)[1] for k in range(1, 16)]
    greeted += [z_at(k) for k in (1, 2, 3, 5, 6, 7)]
    greeted += [y_at(k) for k in range(1, 8)]
    for where in greeted:
        pl.semaphore_signal(barrier, inc=1, device_id=where, device_id_type=MESH)

    loads[0].wait()
    loads[1].wait()
    own_row = pl.multiple_of(me * CAT, CAT)

    def columns(scales):
        for k in range(2):
            for g in range(2):
                lanes[2 * k + g : 2 * k + g + 1, 0:COLS] = scales[k, g : g + 1, :]
        column[...] = jnp.transpose(lanes[...])

    def scaled(codes, k, here):
        parts = [
            codes[k, here, g * QBLOCK : (g + 1) * QBLOCK].astype(F32)
            * column[here, 2 * k + g : 2 * k + g + 1]
            for g in range(2)
        ]
        return jnp.concatenate(parts, axis=1)

    columns(ws)

    def dequantize(first):
        def some(i, carry):
            here = pl.ds(pl.multiple_of(first * 32 + i * 32, 32), 32)
            for k in range(2):
                there = pl.ds(pl.multiple_of(own_row + k * COLS + first * 32 + i * 32, 32), 32)
                wbuf[there, :] = scaled(wc, k, here).astype(BF16)
            return carry

        lax.fori_loop(0, COLS // 64, some, 0)

    weights = Gather(at, wbuf, wtransit, wsend, wrecv, wrelay, wsib)
    dequantize(0)
    pl.semaphore_wait(barrier, len(greeted))
    weights.start_z((0, 1))
    dequantize(COLS // 64)
    weights.start_z((2, 3))
    loads[2].wait()

    own_tokens = pl.ds(pl.multiple_of(y * 32, 32), 32)

    def exchange_tokens(plane):
        for k in range(0 if plane else 1, 8):
            spot = lax.rem(x * 2 + c + k, 8)
            there = (1 - zh if plane else zh) * 8 + spot
            where = {
                "inner_0": there // 8,
                "inner_1": lax.rem(there // 2, 4),
                "inner_2": lax.rem(there, 2),
            }
            pltpu.make_async_remote_copy(
                src_ref=tok.at[own_tokens, pl.ds(pl.multiple_of(there * ROWS, ROWS), ROWS)],
                dst_ref=xt.at[me, y],
                send_sem=xsend.at[plane],
                recv_sem=xrecv.at[plane],
                device_id=where,
                device_id_type=MESH,
            ).start()

    exchange_tokens(0)
    weights.start_x()
    xt[me, y] = tok[own_tokens, pl.ds(pl.multiple_of(me * ROWS, ROWS), ROWS)]

    def share_of(k, plane):
        first = pl.multiple_of((1 - zh if plane else zh) * 8, 8)
        return xt.at[pl.ds(first, 8), lax.rem(y + k, 8)]

    def y_share(k, right, slot, plane):
        share = share_of(k, plane)
        pltpu.make_async_remote_copy(
            src_ref=share,
            dst_ref=share,
            send_sem=ysend,
            recv_sem=yrecv.at[plane * 7 + slot],
            device_id=y_at(1 if right else 7),
            device_id_type=MESH,
        ).start()

    def y_wait(k, slot, plane):
        wait_bytes(share_of(k, plane), yrecv.at[plane * 7 + slot])

    def y_first(plane):
        wait_bytes(xt.at[pl.ds(0, 7 + plane), 0], xrecv.at[plane])
        y_share(0, True, 0, plane)
        y_share(0, False, 4, plane)

    def y_step(s, plane):
        y_wait(8 - s, s - 1, plane)
        if s < 4:
            y_share(8 - s, True, s, plane)
        if s < 4:
            y_wait(s, 3 + s, plane)
        if s < 3:
            y_share(s, False, 4 + s, plane)

    def multiply(role):
        for k, (number, block) in enumerate(weights.blocks(role)):
            mine = tok[:, pl.ds(pl.multiple_of(number * ROWS, ROWS), ROWS)]
            product = lax.dot_general(
                block, mine, (((1,), (1,)), ((), ())), preferred_element_type=F32
            )
            acc[...] = product if role == "own" and k == 0 else acc[...] + product

    multiply("own")
    weights.pass_on(0)
    weights.first_hop()
    weights.pass_on(1)
    weights.pass_on(2)
    weights.near_done()
    exchange_tokens(1)
    weights.pass_on(3)
    y_first(0)
    weights.partner(0)
    multiply("r")
    multiply("l")
    weights.far_done()
    weights.partner(1)
    y_step(1, 0)
    weights.partner_hop(0)
    weights.partner(2)
    multiply("a")
    weights.partner(3)
    weights.partner_hop(1)
    y_step(2, 0)
    y_first(1)
    weights.partner_hop(2)
    multiply("p")
    y_step(3, 0)
    y_step(1, 1)
    weights.partner_hop(3)
    weights.partner_near_done()
    multiply("pl")
    multiply("pr")
    weights.partner_far_done()
    y_step(4, 0)
    multiply("pa")

    loads[3].wait()

    def activate(i, carry):
        here = pl.ds(pl.multiple_of(i * 32, 32), 32)
        gate = acc[here, :]
        up = acc[pl.ds(pl.multiple_of(COLS + i * 32, 32), 32), :]
        back = cot[here, :].astype(F32)
        sig = jax.nn.sigmoid(gate)
        d_gate = back * up * sig * (1.0 + gate * (1.0 - sig))
        d_up = back * gate * sig
        hid[here, :] = (gate * sig * up).astype(BF16)
        for k, value in enumerate((d_gate, d_up)):
            there = pl.ds(pl.multiple_of(own_row + k * COLS + i * 32, 32), 32)
            dbuf[there, :] = value.astype(BF16)
        return carry

    lax.fori_loop(0, COLS // 32, activate, 0)

    deltas = Gather(at, dbuf, dtransit, dsend, drecv, drelay, dsib)
    deltas.start_z(range(4))
    deltas.start_x()

    def partial_inputs(k):
        pair = lax.rem(lax.rem(y + 4, 8) // 2 + k, 4)
        for run in range(4):
            product = jnp.dot(
                own[...], weights.block(run * 4 + pair), preferred_element_type=F32
            ).astype(BF16)
            term[pair * 2, run] = product[:, :128]
            term[pair * 2 + 1, run] = product[:, 128:]

    def target(d, s):
        return lax.rem(y + (4 - s if d == 0 else 4 + s), 8)

    def reduce_send(d, s, h):
        pltpu.make_async_remote_copy(
            src_ref=term.at[target(d, s), pl.ds(h * 2, 2)],
            dst_ref=landed.at[d, s, h],
            send_sem=rsend,
            recv_sem=rrecv.at[(d * 4 + s) * 2 + h],
            device_id=y_at(1 if d == 0 else 7),
            device_id_type=MESH,
        ).start()

    def reduce_wait(d, s, h):
        wait_bytes(landed.at[d, s, h], rrecv.at[(d * 4 + s) * 2 + h])

    def reduce_step(d, s, h):
        reduce_wait(d, s, h)
        goal = target(d, s + 1)

        def add(i, carry):
            here = pl.ds(pl.multiple_of(i * 64, 64), 64)
            for k in range(2):
                came = landed[d, s, h, k, here].astype(F32)
                mine = term[goal, h * 2 + k, here].astype(F32)
                term[goal, h * 2 + k, here] = (mine + came).astype(BF16)
            return carry

        lax.fori_loop(0, ROWS // 64, add, 0)
        reduce_send(d, s + 1, h)

    def reduce_last():
        for h in range(2):
            for d in range(2):
                reduce_wait(d, 3, h)
        for k in (1, 2, 3, 0):
            run = lax.rem(zl + k, 4)

            def add(i, carry, k=k, run=run):
                here = pl.ds(pl.multiple_of(i * 64, 64), 64)
                total = term[y, run, here].astype(F32)
                for d in range(2):
                    total = total + landed[d, 3, run // 2, lax.rem(run, 2), here].astype(F32)
                if k:
                    zsend[k - 1, here] = total.astype(BF16)
                else:
                    igacc[here] = total
                return carry

            lax.fori_loop(0, ROWS // 64, add, 0)
            if k:
                pltpu.make_async_remote_copy(
                    src_ref=zsend.at[k - 1],
                    dst_ref=zland.at[k - 1],
                    send_sem=zs_send,
                    recv_sem=zs_recv,
                    device_id={"outer_0": run},
                    device_id_type=MESH,
                ).start()

    def input_done():
        wait_bytes(zland, zs_recv)

        def add(i, carry):
            here = pl.ds(pl.multiple_of(i * 64, 64), 64)
            total = igacc[here]
            for k in range(3):
                total = total + zland[k, here].astype(F32)
            ig[here] = total.astype(BF16)
            return carry

        lax.fori_loop(0, ROWS // 64, add, 0)

    def accumulate(role):
        for k, (number, block) in enumerate(deltas.blocks(role)):
            product = jnp.dot(
                block, xt[number].reshape(ROWS, ROWS), preferred_element_type=F32
            )
            acc[...] = product if role == "own" and k == 0 else acc[...] + product

    for t in range(CAT // 128):
        there = pl.ds(pl.multiple_of(own_row + t * 128, 128), 128)
        own[:, t * 128 : (t + 1) * 128] = jnp.transpose(dbuf[there, :])
    partial_inputs(0)
    reduce_send(0, 0, 0)
    reduce_send(1, 0, 1)
    partial_inputs(1)
    partial_inputs(3)
    reduce_send(0, 1, 1)
    reduce_send(1, 1, 0)
    y_step(2, 1)
    partial_inputs(2)
    deltas.pass_on(0)
    reduce_step(0, 0, 0)
    reduce_step(1, 0, 1)
    deltas.first_hop()
    deltas.pass_on(1)
    reduce_step(0, 1, 1)
    reduce_step(1, 1, 0)
    deltas.pass_on(2)
    deltas.near_done()
    deltas.pass_on(3)
    y_step(3, 1)
    reduce_step(0, 1, 0)
    reduce_step(1, 1, 1)
    accumulate("own")
    deltas.partner(0)
    reduce_step(0, 2, 1)
    reduce_step(1, 2, 0)
    accumulate("r")
    deltas.far_done()
    deltas.partner(1)
    accumulate("l")
    deltas.partner_hop(0)
    reduce_step(0, 2, 0)
    reduce_step(1, 2, 1)
    deltas.partner(2)
    deltas.partner_hop(1)
    deltas.partner(3)
    accumulate("a")
    y_step(4, 1)
    deltas.partner_hop(2)
    accumulate("p")
    reduce_last()
    deltas.partner_hop(3)
    deltas.partner_near_done()
    accumulate("pl")
    accumulate("pr")
    deltas.partner_far_done()
    accumulate("pa")
    input_done()

    loads[4].wait()
    loads[5].wait()

    columns(gs)

    def totals(i, squares):
        here = pl.ds(pl.multiple_of(i * 32, 32), 32)
        for k in range(2):
            grad = acc[pl.ds(pl.multiple_of(k * COLS + i * 32, 32), 32), :]
            total = scaled(gc, k, here) + grad
            upd[k, here, :] = total
            squares = squares + jnp.sum((total * total).reshape(4, 8, ROWS), axis=0)
        return squares

    squares = lax.fori_loop(0, COLS // 32, totals, jnp.zeros((8, ROWS), F32))
    part[0] = jnp.broadcast_to(jnp.sum(squares, keepdims=True), (8, 128))
    value = part[0]
    for stage, peer in enumerate((plane_at, z_at, y_at)):
        for k in range(1, 8):
            pltpu.make_async_remote_copy(
                src_ref=part.at[stage],
                dst_ref=parts.at[stage, k - 1],
                send_sem=msend.at[stage],
                recv_sem=mrecv.at[stage],
                device_id=peer(k),
                device_id_type=MESH,
            ).start()
        wait_bytes(parts.at[stage], mrecv.at[stage])
        for k in range(7):
            value = value + parts[stage, k]
        if stage < 2:
            part[stage + 1] = value
    scale[...] = 1.0 / jnp.sqrt(value / (2.0 * D * FF) + 1e-06)

    weights.finish()
    deltas.finish()
    for plane in range(2):
        wait_bytes(xt.at[pl.ds(0, 7 + plane), 0], xsend.at[plane])
    wait_bytes(xt.at[:, pl.ds(0, 7)], ysend)
    wait_bytes(term.at[pl.ds(0, 7)], rsend)
    wait_bytes(zsend, zs_send)
    for stage in range(3):
        wait_bytes(parts.at[stage], msend.at[stage])

def finish(hid, ig, total, scale, hid_o, ig_o, upd_o, upd, sem):
    outs = [pltpu.make_async_copy(hid, hid_o, sem.at[0]), pltpu.make_async_copy(ig, ig_o, sem.at[1])]
    for out in outs:
        out.start()
    factor = scale[0:1, 0:1]
    for half in range(2):

        def normalize(i, carry, half=half):
            here = pl.ds(pl.multiple_of(i * 64, 64), 64)
            upd[half, here, :] = total[half, here, :] * factor
            return carry

        lax.fori_loop(0, COLS // 64, normalize, 0)
        out = pltpu.make_async_copy(upd.at[half], upd_o.at[half], sem.at[2 + half])
        out.start()
        outs.append(out)
    for out in outs:
        out.wait()


def local(tokens, weight_codes, weight_scales, grad_codes, grad_scales, cotangent):
    dma = pltpu.SemaphoreType.DMA
    slots = len(GATHER_SLOTS)
    gather = [dma, dma((slots,)), dma((8,)), dma((8,))]
    call = pl.pallas_call(
        kernel,
        out_shape=(
            pltpu.VMEM((COLS, ROWS), BF16),
            pltpu.VMEM((ROWS, 128), BF16),
            pltpu.VMEM((2, COLS, ROWS), F32),
            pltpu.VMEM((8, 128), F32),
        ),
        in_specs=[pl.BlockSpec(memory_space=pltpu.HBM)] * 6,
        out_specs=[pl.BlockSpec(memory_space=pltpu.VMEM)] * 4,
        scratch_shapes=[
            pltpu.VMEM((ROWS, D), BF16),
            pltpu.VMEM((2, COLS, ROWS), jnp.int32),
            pltpu.VMEM((2, 2, COLS), F32),
            pltpu.VMEM((2, COLS, ROWS), jnp.int32),
            pltpu.VMEM((2, 2, COLS), F32),
            pltpu.VMEM((COLS, ROWS), BF16),
            pltpu.VMEM((16 * CAT, ROWS), BF16),
            pltpu.VMEM((16 * CAT, ROWS), BF16),
            pltpu.VMEM((8, PIECE, ROWS), BF16),
            pltpu.VMEM((8, PIECE, ROWS), BF16),
            pltpu.VMEM((16, 8, 32, ROWS), BF16),
            pltpu.VMEM((CAT, ROWS), F32),
            pltpu.VMEM((8, 4, ROWS, 128), BF16),
            pltpu.VMEM((2, 4, 2, 2, ROWS, 128), BF16),
            pltpu.VMEM((3, ROWS, 128), BF16),
            pltpu.VMEM((3, ROWS, 128), BF16),
            pltpu.VMEM((ROWS, 128), F32),
            pltpu.VMEM((ROWS, CAT), BF16),
            pltpu.VMEM((8, 512), F32),
            pltpu.VMEM((512, 8), F32),
            pltpu.VMEM((3, 8, 128), F32),
            pltpu.VMEM((3, 7, 8, 128), F32),
            dma((6,)),
            *gather,
            *gather,
            dma((2,)),
            dma((2,)),
            dma,
            dma((14,)),
            dma,
            dma((16,)),
            dma,
            dma,
            dma((3,)),
            dma((3,)),
        ],
        compiler_params=pltpu.CompilerParams(
            collective_id=0, has_side_effects=True, vmem_limit_bytes=48 * 1024 * 1024
        ),
    )
    given = (
        tokens,
        weight_codes.transpose(0, 2, 1),
        weight_scales,
        grad_codes.transpose(0, 2, 1),
        grad_scales,
        cotangent.T,
    )
    made = call(*(pltpu.with_memory_space_constraint(a, pltpu.HBM) for a in given))
    hidden, input_grad, update = pl.pallas_call(
        finish,
        out_shape=(
            jax.ShapeDtypeStruct((COLS, ROWS), BF16),
            jax.ShapeDtypeStruct((ROWS, 128), BF16),
            jax.ShapeDtypeStruct((2, COLS, ROWS), F32),
        ),
        in_specs=[pl.BlockSpec(memory_space=pltpu.VMEM)] * 4,
        out_specs=[pl.BlockSpec(memory_space=pltpu.HBM)] * 3,
        scratch_shapes=[pltpu.VMEM((2, COLS, ROWS), F32), dma((4,))],
        compiler_params=pltpu.CompilerParams(vmem_limit_bytes=8 * 1024 * 1024),
    )(*made)
    return hidden.T, input_grad, update.transpose(0, 2, 1)


def solution(mesh):
    finer = Mesh(
        mesh.devices.reshape(4, 8, 2, 4, 2), ("outer_0", "outer_1", "inner_0", "inner_1", "inner_2")
    )
    return jax.shard_map(
        local,
        mesh=finer,
        in_specs=(
            P(INNER, None),
            P(None, INNER, OUTER),
            P(None, INNER, OUTER),
            P(None, INNER, OUTER),
            P(None, INNER, OUTER),
            P(INNER, OUTER),
        ),
        out_specs=(P(INNER, OUTER), P(INNER, OUTER), P(None, INNER, OUTER)),
        check_vma=False,
    )
```

```python
import jax
import jax.numpy as jnp
from jax import lax
from jax.experimental import pallas as pl
from jax.experimental.pallas import tpu as pltpu
from jax.sharding import Mesh
from jax.sharding import PartitionSpec as P

D = 4096
FF = 14336
QBLOCK = 128
INNER = ("inner_0", "inner_1", "inner_2")
OUTER = ("outer_0", "outer_1")
ROWS = 256
COLS = 448
CAT = 2 * COLS
MESH = pl.DeviceIdType.MESH
F32 = jnp.float32
BF16 = jnp.bfloat16

CHUNK = COLS // 2
PIECE = COLS // 4

GATHER_SLOTS = {
    name: k
    for k, name in enumerate(
        [f"{b}{g}{j}" for b in ("l", "r", "a") for g in range(2) for j in range(2)]
        + [f"{b}{q}" for b in ("p", "pl", "pr", "pa") for q in range(8)]
    )
}
ROLES = ("own", "r", "l", "a", "p", "pr", "pl", "pa")


def wait_bytes(ref, sem):
    pltpu.make_async_copy(ref, ref, sem).wait()


class Gather:
    def __init__(self, at, buf, transit, send, recv, relay, sib):
        self.at, self.buf, self.transit = at, buf, transit
        self.send, self.recv, self.relay, self.sib = send, recv, relay, sib
        zh, x, c = at["zh"], at["x"], at["c"]

        def chip(h, k):
            return h * 4 + lax.rem(x + k, 4)

        other = 1 - zh
        self.chip = {
            "own": chip(zh, 0),
            "r": chip(zh, 1),
            "a": chip(zh, 2),
            "l": chip(zh, 3),
            "p": chip(other, 0),
            "pr": chip(other, 1),
            "pa": chip(other, 2),
            "pl": chip(other, 3),
        }

    def rows(self, role, first, count, sibling=False):
        c = self.at["c"]
        block = self.chip[role] * 2 + (1 - c if sibling else c)
        return self.buf.at[pl.ds(pl.multiple_of(block * CAT + first, 16), count)]

    def piece(self, role, q):
        return self.rows(role, q * PIECE, PIECE)

    def copy(self, src, dst, recv, where):
        pltpu.make_async_remote_copy(
            src_ref=src,
            dst_ref=dst,
            send_sem=self.send,
            recv_sem=recv,
            device_id=where,
            device_id_type=MESH,
        ).start()

    def along_x(self, part, right, slot):
        where = {"inner_1": self.at["right"] if right else self.at["left"]}
        self.copy(part, part, self.recv.at[GATHER_SLOTS[slot]], where)

    def part(self, role, g, j, sibling=False):
        return self.rows(role, g * COLS + j * CHUNK, CHUNK, sibling)

    def along_z(self, q):
        where = self.at["up2"] if q < 4 else self.at["down2"]
        self.copy(self.piece("own", q), self.transit.at[q], self.relay.at[q], where)

    def pass_on(self, k):
        at = self.at
        for q in (k, k + 4):
            wait_bytes(self.transit.at[q], self.relay.at[q])
            origin = at["down2"] if q < 4 else at["up2"]
            where = at["up2"] if q < 4 else at["down2"]
            block = (origin["inner_0"] * 4 + at["x"]) * 2 + at["c"]
            dst = self.buf.at[pl.ds(pl.multiple_of(block * CAT + q * PIECE, 16), PIECE)]
            self.copy(self.transit.at[q], dst, self.recv.at[GATHER_SLOTS[f"p{q}"]], where)

    def sibling_sem(self, role, g, j):
        return self.sib.at[(ROLES.index(role) * 2 + j) * 2 + g]

    def to_sibling(self, role, j):
        for g in range(2):
            part = self.part(role, g, j)
            self.copy(part, part, self.sibling_sem(role, g, j), {"inner_2": 1 - self.at["c"]})

    def start_z(self, ks):
        for k in ks:
            self.along_z(k)
            self.along_z(k + 4)

    def start_x(self, j):
        self.along_x(self.part("own", 0, j), True, f"l0{j}")
        self.along_x(self.part("own", 1, j), False, f"r1{j}")
        self.along_x(self.part("own", 1, j), True, f"l1{j}")
        self.along_x(self.part("own", 0, j), False, f"r0{j}")
        self.to_sibling("own", j)

    def wait_part(self, role, g, j):
        wait_bytes(self.part(role, g, j), self.recv.at[GATHER_SLOTS[f"{role}{g}{j}"]])

    def wait_piece(self, role, q):
        wait_bytes(self.piece(role, q), self.recv.at[GATHER_SLOTS[f"{role}{q}"]])

    def first_hop(self, j):
        self.wait_part("l", 0, j)
        self.along_x(self.part("l", 0, j), True, f"a0{j}")
        self.wait_part("r", 1, j)
        self.along_x(self.part("r", 1, j), False, f"a1{j}")

    def near_done(self, j):
        self.wait_part("l", 1, j)
        self.to_sibling("l", j)
        self.wait_part("r", 0, j)
        self.to_sibling("r", j)

    def far_done(self, j):
        self.wait_part("a", 0, j)
        self.wait_part("a", 1, j)
        self.to_sibling("a", j)

    def partner(self, k):
        for q in (k, k + 4):
            self.wait_piece("p", q)
            self.along_x(self.piece("p", q), True, f"pl{q}")
            self.along_x(self.piece("p", q), False, f"pr{q}")
        if k % 2 == 1:
            self.to_sibling("p", k // 2)

    def partner_hop(self, k):
        self.wait_piece("pl", k)
        self.along_x(self.piece("pl", k), True, f"pa{k}")
        self.wait_piece("pr", k + 4)
        self.along_x(self.piece("pr", k + 4), False, f"pa{k + 4}")

    def partner_near_done(self, j):
        for q in (4 + 2 * j, 5 + 2 * j):
            self.wait_piece("pl", q)
        self.to_sibling("pl", j)
        for q in (2 * j, 2 * j + 1):
            self.wait_piece("pr", q)
        self.to_sibling("pr", j)

    def partner_far_done(self, j):
        for k in (2 * j, 2 * j + 1):
            self.wait_piece("pa", k)
            self.wait_piece("pa", k + 4)
        self.to_sibling("pa", j)

    def blocks(self, role, j):
        c = self.at["c"]
        for k, which in enumerate((c, 1 - c)):
            parts = [self.part(role, g, j, k == 1) for g in range(2)]
            if k:
                for g in range(2):
                    wait_bytes(parts[g], self.sibling_sem(role, g, j))
            yield self.chip[role] * 2 + which, jnp.concatenate([p[...] for p in parts], axis=0)

    def block(self, number):
        return self.buf[pl.ds(pl.multiple_of(number * CAT, CAT), CAT), :]

    def finish(self):
        wait_bytes(self.buf, self.send)


def kernel(
    tok_h,
    wc_h,
    ws_h,
    gc_h,
    gs_h,
    cot_h,
    hid,
    ig,
    upd,
    scale,
    tok,
    wc,
    ws,
    gc,
    gs,
    cot,
    wbuf,
    dbuf,
    wtransit,
    dtransit,
    xt,
    acc,
    term,
    landed,
    zsend,
    zland,
    igacc,
    own,
    lanes,
    column,
    part,
    parts,
    load_sem,
    wsend,
    wrecv,
    wrelay,
    wsib,
    dsend,
    drecv,
    drelay,
    dsib,
    xsend,
    xrecv,
    ysend,
    yrecv,
    rsend,
    rrecv,
    zs_send,
    zs_recv,
    msend,
    mrecv,
):
    zl, y = lax.axis_index("outer_0"), lax.axis_index("outer_1")
    zh, x, c = (lax.axis_index(a) for a in INNER)
    z = zh * 4 + zl
    me = (zh * 4 + x) * 2 + c

    def z_at(k):
        there = lax.rem(z + k, 8)
        return {"outer_0": lax.rem(there, 4), "inner_0": there // 4}

    def inner_at(k):
        there = lax.rem(me + k, 16)
        return there, {
            "inner_0": there // 8,
            "inner_1": lax.rem(there // 2, 4),
            "inner_2": lax.rem(there, 2),
        }

    def plane_at(k):
        there = lax.rem(x * 2 + c + k, 8)
        return {"inner_1": there // 2, "inner_2": lax.rem(there, 2)}

    def y_at(k):
        return {"outer_1": lax.rem(y + k, 8)}

    at = {
        "zh": zh,
        "x": x,
        "c": c,
        "right": lax.rem(x + 1, 4),
        "left": lax.rem(x + 3, 4),
        "up2": z_at(2),
        "down2": z_at(6),
    }

    loads = [
        pltpu.make_async_copy(src, dst, load_sem.at[k])
        for k, (src, dst) in enumerate(
            ((ws_h, ws), (wc_h, wc), (tok_h, tok), (cot_h, cot), (gs_h, gs), (gc_h, gc))
        )
    ]
    for load in loads:
        load.start()

    barrier = pltpu.get_barrier_semaphore()
    greeted = [inner_at(k)[1] for k in range(1, 16)]
    greeted += [z_at(k) for k in (1, 2, 3, 5, 6, 7)]
    greeted += [y_at(k) for k in range(1, 8)]
    for where in greeted:
        pl.semaphore_signal(barrier, inc=1, device_id=where, device_id_type=MESH)

    loads[0].wait()
    loads[1].wait()
    own_row = pl.multiple_of(me * CAT, CAT)

    def columns(scales):
        for k in range(2):
            for g in range(2):
                lanes[2 * k + g : 2 * k + g + 1, 0:COLS] = scales[k, g : g + 1, :]
        column[...] = jnp.transpose(lanes[...])

    def scaled(codes, k, here):
        parts = [
            codes[k, here, g * QBLOCK : (g + 1) * QBLOCK].astype(F32)
            * column[here, 2 * k + g : 2 * k + g + 1]
            for g in range(2)
        ]
        return jnp.concatenate(parts, axis=1)

    columns(ws)

    def dequantize(first):
        def some(i, carry):
            here = pl.ds(pl.multiple_of(first * 32 + i * 32, 32), 32)
            for k in range(2):
                there = pl.ds(pl.multiple_of(own_row + k * COLS + first * 32 + i * 32, 32), 32)
                wbuf[there, :] = scaled(wc, k, here).astype(BF16)
            return carry

        lax.fori_loop(0, COLS // 64, some, 0)

    weights = Gather(at, wbuf, wtransit, wsend, wrecv, wrelay, wsib)
    dequantize(0)
    pl.semaphore_wait(barrier, len(greeted))
    weights.start_z((0, 1))
    weights.start_x(0)
    dequantize(COLS // 64)
    weights.start_z((2, 3))
    loads[2].wait()

    own_tokens = pl.ds(pl.multiple_of(y * 32, 32), 32)

    def exchange_tokens(plane):
        for k in range(0 if plane else 1, 8):
            spot = lax.rem(x * 2 + c + k, 8)
            there = (1 - zh if plane else zh) * 8 + spot
            where = {
                "inner_0": there // 8,
                "inner_1": lax.rem(there // 2, 4),
                "inner_2": lax.rem(there, 2),
            }
            pltpu.make_async_remote_copy(
                src_ref=tok.at[own_tokens, pl.ds(pl.multiple_of(there * ROWS, ROWS), ROWS)],
                dst_ref=xt.at[me, y],
                send_sem=xsend.at[plane],
                recv_sem=xrecv.at[plane],
                device_id=where,
                device_id_type=MESH,
            ).start()

    exchange_tokens(0)
    weights.start_x(1)
    xt[me, y] = tok[own_tokens, pl.ds(pl.multiple_of(me * ROWS, ROWS), ROWS)]

    def share_of(k, plane):
        first = pl.multiple_of((1 - zh if plane else zh) * 8, 8)
        return xt.at[pl.ds(first, 8), lax.rem(y + k, 8)]

    def y_share(k, right, slot, plane):
        share = share_of(k, plane)
        pltpu.make_async_remote_copy(
            src_ref=share,
            dst_ref=share,
            send_sem=ysend,
            recv_sem=yrecv.at[plane * 7 + slot],
            device_id=y_at(1 if right else 7),
            device_id_type=MESH,
        ).start()

    def y_wait(k, slot, plane):
        wait_bytes(share_of(k, plane), yrecv.at[plane * 7 + slot])

    def y_first(plane):
        wait_bytes(xt.at[pl.ds(0, 7 + plane), 0], xrecv.at[plane])
        y_share(0, True, 0, plane)
        y_share(0, False, 4, plane)

    def y_step(s, plane):
        y_wait(8 - s, s - 1, plane)
        if s < 4:
            y_share(8 - s, True, s, plane)
        if s < 4:
            y_wait(s, 3 + s, plane)
        if s < 3:
            y_share(s, False, 4 + s, plane)

    def multiply(role, j):
        for k, (number, block) in enumerate(weights.blocks(role, j)):
            mine = tok[:, pl.ds(pl.multiple_of(number * ROWS, ROWS), ROWS)]
            product = lax.dot_general(
                block, mine, (((1,), (1,)), ((), ())), preferred_element_type=F32
            )
            acc[j] = product if role == "own" and k == 0 else acc[j] + product

    def activate(j):
        def some(i, carry):
            here = pl.ds(pl.multiple_of(j * CHUNK + i * 32, 32), 32)
            gate = acc[j, pl.ds(pl.multiple_of(i * 32, 32), 32), :]
            up = acc[j, pl.ds(pl.multiple_of(CHUNK + i * 32, 32), 32), :]
            back = cot[here, :].astype(F32)
            sig = jax.nn.sigmoid(gate)
            d_gate = back * up * sig * (1.0 + gate * (1.0 - sig))
            d_up = back * gate * sig
            hid[here, :] = (gate * sig * up).astype(BF16)
            for k, value in enumerate((d_gate, d_up)):
                there = pl.ds(
                    pl.multiple_of(own_row + k * COLS + j * CHUNK + i * 32, 32), 32
                )
                dbuf[there, :] = value.astype(BF16)
            return carry

        lax.fori_loop(0, CHUNK // 32, some, 0)

    deltas = Gather(at, dbuf, dtransit, dsend, drecv, drelay, dsib)

    def partial_inputs(k):
        pair = lax.rem(lax.rem(y + 4, 8) // 2 + k, 4)
        for run in range(4):
            product = jnp.dot(
                own[...], weights.block(run * 4 + pair), preferred_element_type=F32
            ).astype(BF16)
            term[pair * 2, run] = product[:, :128]
            term[pair * 2 + 1, run] = product[:, 128:]

    def target(d, s):
        return lax.rem(y + (4 - s if d == 0 else 4 + s), 8)

    def reduce_send(d, s, h):
        pltpu.make_async_remote_copy(
            src_ref=term.at[target(d, s), pl.ds(h * 2, 2)],
            dst_ref=landed.at[d, s, h],
            send_sem=rsend,
            recv_sem=rrecv.at[(d * 4 + s) * 2 + h],
            device_id=y_at(1 if d == 0 else 7),
            device_id_type=MESH,
        ).start()

    def reduce_wait(d, s, h):
        wait_bytes(landed.at[d, s, h], rrecv.at[(d * 4 + s) * 2 + h])

    def reduce_step(d, s, h):
        reduce_wait(d, s, h)
        goal = target(d, s + 1)

        def add(i, carry):
            here = pl.ds(pl.multiple_of(i * 64, 64), 64)
            for k in range(2):
                came = landed[d, s, h, k, here].astype(F32)
                mine = term[goal, h * 2 + k, here].astype(F32)
                term[goal, h * 2 + k, here] = (mine + came).astype(BF16)
            return carry

        lax.fori_loop(0, ROWS // 64, add, 0)
        reduce_send(d, s + 1, h)

    def reduce_last():
        for h in range(2):
            for d in range(2):
                reduce_wait(d, 3, h)
        for k in (1, 2, 3, 0):
            run = lax.rem(zl + k, 4)

            def add(i, carry, k=k, run=run):
                here = pl.ds(pl.multiple_of(i * 64, 64), 64)
                total = term[y, run, here].astype(F32)
                for d in range(2):
                    total = total + landed[d, 3, run // 2, lax.rem(run, 2), here].astype(F32)
                if k:
                    zsend[k - 1, here] = total.astype(BF16)
                else:
                    igacc[here] = total
                return carry

            lax.fori_loop(0, ROWS // 64, add, 0)
            if k:
                pltpu.make_async_remote_copy(
                    src_ref=zsend.at[k - 1],
                    dst_ref=zland.at[k - 1],
                    send_sem=zs_send,
                    recv_sem=zs_recv,
                    device_id={"outer_0": run},
                    device_id_type=MESH,
                ).start()

    def input_done():
        wait_bytes(zland, zs_recv)

        def add(i, carry):
            here = pl.ds(pl.multiple_of(i * 64, 64), 64)
            total = igacc[here]
            for k in range(3):
                total = total + zland[k, here].astype(F32)
            ig[here] = total.astype(BF16)
            return carry

        lax.fori_loop(0, ROWS // 64, add, 0)

    def accumulate(role, j):
        for k, (number, block) in enumerate(deltas.blocks(role, j)):
            product = jnp.dot(
                block, xt[number].reshape(ROWS, ROWS), preferred_element_type=F32
            )
            acc[j] = product if role == "own" and k == 0 else acc[j] + product

    def totals(j, squares):
        def some(i, squares):
            here = pl.ds(pl.multiple_of(j * CHUNK + i * 32, 32), 32)
            for k in range(2):
                grad = acc[j, pl.ds(pl.multiple_of(k * CHUNK + i * 32, 32), 32), :]
                total = scaled(gc, k, here) + grad
                upd[k, here, :] = total
                squares = squares + jnp.sum((total * total).reshape(4, 8, ROWS), axis=0)
            return squares

        return lax.fori_loop(0, CHUNK // 32, some, squares)

    multiply("own", 0)
    weights.first_hop(0)
    multiply("own", 1)
    weights.pass_on(0)
    weights.near_done(0)
    weights.pass_on(1)
    weights.first_hop(1)
    weights.pass_on(2)
    weights.near_done(1)
    weights.pass_on(3)
    multiply("r", 0)
    multiply("l", 0)
    y_first(0)
    weights.far_done(0)
    weights.partner(0)
    multiply("r", 1)
    multiply("l", 1)
    weights.far_done(1)
    weights.partner(1)
    y_step(1, 0)
    multiply("a", 0)
    weights.partner_hop(0)
    weights.partner(2)
    exchange_tokens(1)
    multiply("a", 1)
    y_step(2, 0)
    weights.partner_hop(1)
    weights.partner(3)
    multiply("p", 0)
    weights.partner_near_done(0)
    multiply("pl", 0)
    multiply("pr", 0)
    weights.partner_far_done(0)
    weights.partner_hop(2)
    y_step(3, 0)
    loads[3].wait()
    multiply("pa", 0)
    activate(0)
    deltas.start_z((0, 1))
    deltas.start_x(0)
    y_first(1)
    weights.partner_hop(3)
    multiply("p", 1)
    weights.partner_near_done(1)
    y_step(4, 0)
    multiply("pl", 1)
    multiply("pr", 1)
    deltas.pass_on(0)
    deltas.first_hop(0)
    weights.partner_far_done(1)
    y_step(1, 1)
    multiply("pa", 1)
    activate(1)
    deltas.start_z((2, 3))
    deltas.start_x(1)

    for t in range(CAT // 128):
        there = pl.ds(pl.multiple_of(own_row + t * 128, 128), 128)
        own[:, t * 128 : (t + 1) * 128] = jnp.transpose(dbuf[there, :])
    partial_inputs(0)
    reduce_send(0, 0, 0)
    reduce_send(1, 0, 1)
    deltas.pass_on(1)
    deltas.near_done(0)
    partial_inputs(1)
    partial_inputs(3)
    reduce_send(0, 1, 1)
    reduce_send(1, 1, 0)
    y_step(2, 1)
    deltas.far_done(0)
    deltas.partner(0)
    partial_inputs(2)
    deltas.first_hop(1)
    deltas.partner(1)
    deltas.pass_on(2)
    reduce_step(0, 0, 0)
    reduce_step(1, 0, 1)
    accumulate("own", 0)
    accumulate("r", 0)
    accumulate("l", 0)
    deltas.near_done(1)
    deltas.pass_on(3)
    y_step(3, 1)
    deltas.partner_hop(0)
    reduce_step(0, 1, 1)
    reduce_step(1, 1, 0)
    accumulate("own", 1)
    accumulate("a", 0)
    deltas.far_done(1)
    deltas.partner(2)
    deltas.partner_hop(1)
    reduce_step(0, 1, 0)
    reduce_step(1, 1, 1)
    accumulate("r", 1)
    accumulate("l", 1)
    deltas.partner(3)
    y_step(4, 1)
    deltas.partner_near_done(0)
    reduce_step(0, 2, 1)
    reduce_step(1, 2, 0)
    accumulate("a", 1)
    accumulate("p", 0)
    deltas.partner_hop(2)
    deltas.partner_far_done(0)
    accumulate("pl", 0)
    accumulate("pr", 0)
    reduce_step(0, 2, 0)
    reduce_step(1, 2, 1)
    accumulate("pa", 0)
    deltas.partner_hop(3)
    accumulate("p", 1)
    loads[4].wait()
    loads[5].wait()
    columns(gs)
    deltas.partner_near_done(1)
    squares = totals(0, jnp.zeros((8, ROWS), F32))
    accumulate("pl", 1)
    accumulate("pr", 1)
    deltas.partner_far_done(1)
    reduce_last()
    accumulate("pa", 1)
    squares = totals(1, squares)
    part[0] = jnp.broadcast_to(jnp.sum(squares, keepdims=True), (8, 128))
    value = part[0]
    for stage, peer in enumerate((plane_at, z_at, y_at)):
        for k in range(1, 8):
            pltpu.make_async_remote_copy(
                src_ref=part.at[stage],
                dst_ref=parts.at[stage, k - 1],
                send_sem=msend.at[stage],
                recv_sem=mrecv.at[stage],
                device_id=peer(k),
                device_id_type=MESH,
            ).start()
        wait_bytes(parts.at[stage], mrecv.at[stage])
        for k in range(7):
            value = value + parts[stage, k]
        if stage < 2:
            part[stage + 1] = value
    input_done()
    scale[...] = 1.0 / jnp.sqrt(value / (2.0 * D * FF) + 1e-06)

    weights.finish()
    deltas.finish()
    for plane in range(2):
        wait_bytes(xt.at[pl.ds(0, 7 + plane), 0], xsend.at[plane])
    wait_bytes(xt.at[:, pl.ds(0, 7)], ysend)
    wait_bytes(term.at[pl.ds(0, 7)], rsend)
    wait_bytes(zsend, zs_send)
    for stage in range(3):
        wait_bytes(parts.at[stage], msend.at[stage])

def finish(hid, ig, total, scale, hid_o, ig_o, upd_o, upd, sem):
    outs = [pltpu.make_async_copy(hid, hid_o, sem.at[0]), pltpu.make_async_copy(ig, ig_o, sem.at[1])]
    for out in outs:
        out.start()
    factor = scale[0:1, 0:1]
    for half in range(2):

        def normalize(i, carry, half=half):
            here = pl.ds(pl.multiple_of(i * 64, 64), 64)
            upd[half, here, :] = total[half, here, :] * factor
            return carry

        lax.fori_loop(0, COLS // 64, normalize, 0)
        out = pltpu.make_async_copy(upd.at[half], upd_o.at[half], sem.at[2 + half])
        out.start()
        outs.append(out)
    for out in outs:
        out.wait()


def local(tokens, weight_codes, weight_scales, grad_codes, grad_scales, cotangent):
    dma = pltpu.SemaphoreType.DMA
    slots = len(GATHER_SLOTS)
    gather = [dma, dma((slots,)), dma((8,)), dma((32,))]
    call = pl.pallas_call(
        kernel,
        out_shape=(
            pltpu.VMEM((COLS, ROWS), BF16),
            pltpu.VMEM((ROWS, 128), BF16),
            pltpu.VMEM((2, COLS, ROWS), F32),
            pltpu.VMEM((8, 128), F32),
        ),
        in_specs=[pl.BlockSpec(memory_space=pltpu.HBM)] * 6,
        out_specs=[pl.BlockSpec(memory_space=pltpu.VMEM)] * 4,
        scratch_shapes=[
            pltpu.VMEM((ROWS, D), BF16),
            pltpu.VMEM((2, COLS, ROWS), jnp.int32),
            pltpu.VMEM((2, 2, COLS), F32),
            pltpu.VMEM((2, COLS, ROWS), jnp.int32),
            pltpu.VMEM((2, 2, COLS), F32),
            pltpu.VMEM((COLS, ROWS), BF16),
            pltpu.VMEM((16 * CAT, ROWS), BF16),
            pltpu.VMEM((16 * CAT, ROWS), BF16),
            pltpu.VMEM((8, PIECE, ROWS), BF16),
            pltpu.VMEM((8, PIECE, ROWS), BF16),
            pltpu.VMEM((16, 8, 32, ROWS), BF16),
            pltpu.VMEM((2, COLS, ROWS), F32),
            pltpu.VMEM((8, 4, ROWS, 128), BF16),
            pltpu.VMEM((2, 4, 2, 2, ROWS, 128), BF16),
            pltpu.VMEM((3, ROWS, 128), BF16),
            pltpu.VMEM((3, ROWS, 128), BF16),
            pltpu.VMEM((ROWS, 128), F32),
            pltpu.VMEM((ROWS, CAT), BF16),
            pltpu.VMEM((8, 512), F32),
            pltpu.VMEM((512, 8), F32),
            pltpu.VMEM((3, 8, 128), F32),
            pltpu.VMEM((3, 7, 8, 128), F32),
            dma((6,)),
            *gather,
            *gather,
            dma((2,)),
            dma((2,)),
            dma,
            dma((14,)),
            dma,
            dma((16,)),
            dma,
            dma,
            dma((3,)),
            dma((3,)),
        ],
        compiler_params=pltpu.CompilerParams(
            collective_id=0, has_side_effects=True, vmem_limit_bytes=48 * 1024 * 1024
        ),
    )
    given = (
        tokens,
        weight_codes.transpose(0, 2, 1),
        weight_scales,
        grad_codes.transpose(0, 2, 1),
        grad_scales,
        cotangent.T,
    )
    made = call(*(pltpu.with_memory_space_constraint(a, pltpu.HBM) for a in given))
    hidden, input_grad, update = pl.pallas_call(
        finish,
        out_shape=(
            jax.ShapeDtypeStruct((COLS, ROWS), BF16),
            jax.ShapeDtypeStruct((ROWS, 128), BF16),
            jax.ShapeDtypeStruct((2, COLS, ROWS), F32),
        ),
        in_specs=[pl.BlockSpec(memory_space=pltpu.VMEM)] * 4,
        out_specs=[pl.BlockSpec(memory_space=pltpu.HBM)] * 3,
        scratch_shapes=[pltpu.VMEM((2, COLS, ROWS), F32), dma((4,))],
        compiler_params=pltpu.CompilerParams(vmem_limit_bytes=8 * 1024 * 1024),
    )(*made)
    return hidden.T, input_grad, update.transpose(0, 2, 1)


def solution(mesh):
    finer = Mesh(
        mesh.devices.reshape(4, 8, 2, 4, 2), ("outer_0", "outer_1", "inner_0", "inner_1", "inner_2")
    )
    return jax.shard_map(
        local,
        mesh=finer,
        in_specs=(
            P(INNER, None),
            P(None, INNER, OUTER),
            P(None, INNER, OUTER),
            P(None, INNER, OUTER),
            P(None, INNER, OUTER),
            P(INNER, OUTER),
        ),
        out_specs=(P(INNER, OUTER), P(INNER, OUTER), P(None, INNER, OUTER)),
        check_vma=False,
    )
```

```python
import jax
import jax.numpy as jnp
from jax import lax
from jax.experimental import pallas as pl
from jax.experimental.pallas import tpu as pltpu
from jax.sharding import Mesh
from jax.sharding import PartitionSpec as P

D = 4096
FF = 14336
QBLOCK = 128
INNER = ("inner_0", "inner_1", "inner_2")
OUTER = ("outer_0", "outer_1")
ROWS = 256
COLS = 448
CAT = 2 * COLS
MESH = pl.DeviceIdType.MESH
F32 = jnp.float32
BF16 = jnp.bfloat16

CHUNK = COLS // 2
PIECE = COLS // 4

GATHER_SLOTS = {
    name: k
    for k, name in enumerate(
        [f"{b}{g}{j}" for b in ("l", "r", "a") for g in range(2) for j in range(2)]
        + [f"{b}{q}" for b in ("p", "pl", "pr", "pa") for q in range(8)]
    )
}
ROLES = ("own", "r", "l", "a", "p", "pr", "pl", "pa")


def wait_bytes(ref, sem):
    pltpu.make_async_copy(ref, ref, sem).wait()


class Gather:
    def __init__(self, at, buf, transit, send, recv, relay, sib):
        self.at, self.buf, self.transit = at, buf, transit
        self.send, self.recv, self.relay, self.sib = send, recv, relay, sib
        zh, x, c = at["zh"], at["x"], at["c"]

        def chip(h, k):
            return h * 4 + lax.rem(x + k, 4)

        other = 1 - zh
        self.chip = {
            "own": chip(zh, 0),
            "r": chip(zh, 1),
            "a": chip(zh, 2),
            "l": chip(zh, 3),
            "p": chip(other, 0),
            "pr": chip(other, 1),
            "pa": chip(other, 2),
            "pl": chip(other, 3),
        }

    def rows(self, role, first, count, sibling=False):
        c = self.at["c"]
        block = self.chip[role] * 2 + (1 - c if sibling else c)
        return self.buf.at[pl.ds(pl.multiple_of(block * CAT + first, 16), count)]

    def piece(self, role, q):
        return self.rows(role, q * PIECE, PIECE)

    def copy(self, src, dst, recv, where):
        pltpu.make_async_remote_copy(
            src_ref=src,
            dst_ref=dst,
            send_sem=self.send,
            recv_sem=recv,
            device_id=where,
            device_id_type=MESH,
        ).start()

    def along_x(self, part, right, slot):
        where = {"inner_1": self.at["right"] if right else self.at["left"]}
        self.copy(part, part, self.recv.at[GATHER_SLOTS[slot]], where)

    def part(self, role, g, j, sibling=False):
        return self.rows(role, g * COLS + j * CHUNK, CHUNK, sibling)

    def along_z(self, q):
        where = self.at["up2"] if q < 4 else self.at["down2"]
        self.copy(self.piece("own", q), self.transit.at[q], self.relay.at[q], where)

    def pass_on(self, k):
        at = self.at
        for q in (k, k + 4):
            wait_bytes(self.transit.at[q], self.relay.at[q])
            origin = at["down2"] if q < 4 else at["up2"]
            where = at["up2"] if q < 4 else at["down2"]
            block = (origin["inner_0"] * 4 + at["x"]) * 2 + at["c"]
            dst = self.buf.at[pl.ds(pl.multiple_of(block * CAT + q * PIECE, 16), PIECE)]
            self.copy(self.transit.at[q], dst, self.recv.at[GATHER_SLOTS[f"p{q}"]], where)

    def sibling_sem(self, role, g, j):
        return self.sib.at[(ROLES.index(role) * 2 + j) * 2 + g]

    def to_sibling(self, role, j):
        for g in range(2):
            part = self.part(role, g, j)
            self.copy(part, part, self.sibling_sem(role, g, j), {"inner_2": 1 - self.at["c"]})

    def start_z(self, ks):
        for k in ks:
            self.along_z(k)
            self.along_z(k + 4)

    def start_x(self, j):
        self.along_x(self.part("own", 0, j), True, f"l0{j}")
        self.along_x(self.part("own", 1, j), False, f"r1{j}")
        self.along_x(self.part("own", 1, j), True, f"l1{j}")
        self.along_x(self.part("own", 0, j), False, f"r0{j}")
        self.to_sibling("own", j)

    def wait_part(self, role, g, j):
        wait_bytes(self.part(role, g, j), self.recv.at[GATHER_SLOTS[f"{role}{g}{j}"]])

    def wait_piece(self, role, q):
        wait_bytes(self.piece(role, q), self.recv.at[GATHER_SLOTS[f"{role}{q}"]])

    def first_hop(self, j):
        self.wait_part("l", 0, j)
        self.along_x(self.part("l", 0, j), True, f"a0{j}")
        self.wait_part("r", 1, j)
        self.along_x(self.part("r", 1, j), False, f"a1{j}")

    def near_done(self, j):
        self.wait_part("l", 1, j)
        self.to_sibling("l", j)
        self.wait_part("r", 0, j)
        self.to_sibling("r", j)

    def far_done(self, j):
        self.wait_part("a", 0, j)
        self.wait_part("a", 1, j)
        self.to_sibling("a", j)

    def partner(self, k):
        for q in (k, k + 4):
            self.wait_piece("p", q)
            self.along_x(self.piece("p", q), True, f"pl{q}")
            self.along_x(self.piece("p", q), False, f"pr{q}")
        if k % 2 == 1:
            self.to_sibling("p", k // 2)

    def partner_hop(self, k):
        self.wait_piece("pl", k)
        self.along_x(self.piece("pl", k), True, f"pa{k}")
        self.wait_piece("pr", k + 4)
        self.along_x(self.piece("pr", k + 4), False, f"pa{k + 4}")

    def partner_near_done(self, j):
        for q in (4 + 2 * j, 5 + 2 * j):
            self.wait_piece("pl", q)
        self.to_sibling("pl", j)
        for q in (2 * j, 2 * j + 1):
            self.wait_piece("pr", q)
        self.to_sibling("pr", j)

    def partner_far_done(self, j):
        for k in (2 * j, 2 * j + 1):
            self.wait_piece("pa", k)
            self.wait_piece("pa", k + 4)
        self.to_sibling("pa", j)

    def blocks(self, role, j):
        c = self.at["c"]
        for k, which in enumerate((c, 1 - c)):
            parts = [self.part(role, g, j, k == 1) for g in range(2)]
            if k:
                for g in range(2):
                    wait_bytes(parts[g], self.sibling_sem(role, g, j))
            yield self.chip[role] * 2 + which, jnp.concatenate([p[...] for p in parts], axis=0)

    def block(self, number):
        return self.buf[pl.ds(pl.multiple_of(number * CAT, CAT), CAT), :]

    def finish(self):
        wait_bytes(self.buf, self.send)


def kernel(
    tok_h,
    wc_h,
    ws_h,
    gc_h,
    gs_h,
    cot_h,
    hid,
    ig,
    upd,
    scale,
    tok,
    wc,
    ws,
    gc,
    gs,
    cot,
    wbuf,
    dbuf,
    wtransit,
    dtransit,
    xt,
    acc,
    term,
    landed,
    zsend,
    zland,
    igacc,
    own,
    lanes,
    column,
    part,
    parts,
    load_sem,
    wsend,
    wrecv,
    wrelay,
    wsib,
    dsend,
    drecv,
    drelay,
    dsib,
    xsend,
    xrecv,
    ysend,
    yrecv,
    rsend,
    rrecv,
    zs_send,
    zs_recv,
    msend,
    mrecv,
):
    zl, y = lax.axis_index("outer_0"), lax.axis_index("outer_1")
    zh, x, c = (lax.axis_index(a) for a in INNER)
    z = zh * 4 + zl
    me = (zh * 4 + x) * 2 + c

    def z_at(k):
        there = lax.rem(z + k, 8)
        return {"outer_0": lax.rem(there, 4), "inner_0": there // 4}

    def plane_at(k):
        there = lax.rem(x * 2 + c + k, 8)
        return {"inner_1": there // 2, "inner_2": lax.rem(there, 2)}

    def y_at(k):
        return {"outer_1": lax.rem(y + k, 8)}

    at = {
        "zh": zh,
        "x": x,
        "c": c,
        "right": lax.rem(x + 1, 4),
        "left": lax.rem(x + 3, 4),
        "up2": z_at(2),
        "down2": z_at(6),
    }

    loads = [
        pltpu.make_async_copy(src, dst, load_sem.at[k])
        for k, (src, dst) in enumerate(
            ((ws_h, ws), (wc_h, wc), (tok_h, tok), (cot_h, cot), (gs_h, gs), (gc_h, gc))
        )
    ]
    for load in loads[:2]:
        load.start()

    barrier = pltpu.get_barrier_semaphore()
    greeted = [plane_at(k) for k in range(1, 8)]
    greeted += [z_at(k) for k in (1, 2, 6, 7)]
    greeted += [y_at(k) for k in (1, 7)]
    for where in greeted:
        pl.semaphore_signal(barrier, inc=1, device_id=where, device_id_type=MESH)

    for load in loads[2:]:
        load.start()

    loads[0].wait()
    loads[1].wait()
    own_row = pl.multiple_of(me * CAT, CAT)

    def columns(scales):
        for k in range(2):
            for g in range(2):
                lanes[2 * k + g : 2 * k + g + 1, 0:COLS] = scales[k, g : g + 1, :]
        column[...] = jnp.transpose(lanes[...])

    def scaled(codes, k, here):
        parts = [
            codes[k, here, g * QBLOCK : (g + 1) * QBLOCK].astype(F32)
            * column[here, 2 * k + g : 2 * k + g + 1]
            for g in range(2)
        ]
        return jnp.concatenate(parts, axis=1)

    columns(ws)

    def dequantize(first):
        def some(i, carry):
            here = pl.ds(pl.multiple_of(first * 32 + i * 32, 32), 32)
            for k in range(2):
                there = pl.ds(pl.multiple_of(own_row + k * COLS + first * 32 + i * 32, 32), 32)
                wbuf[there, :] = scaled(wc, k, here).astype(BF16)
            return carry

        lax.fori_loop(0, COLS // 64, some, 0)

    weights = Gather(at, wbuf, wtransit, wsend, wrecv, wrelay, wsib)
    dequantize(0)
    pl.semaphore_wait(barrier, len(greeted))
    weights.start_z((0, 1))
    weights.start_x(0)
    dequantize(COLS // 64)
    weights.start_z((2, 3))
    loads[2].wait()

    own_tokens = pl.ds(pl.multiple_of(y * 32, 32), 32)

    def exchange_tokens(plane):
        for k in range(0 if plane else 1, 8):
            spot = lax.rem(x * 2 + c + k, 8)
            there = (1 - zh if plane else zh) * 8 + spot
            where = {
                "inner_0": there // 8,
                "inner_1": lax.rem(there // 2, 4),
                "inner_2": lax.rem(there, 2),
            }
            pltpu.make_async_remote_copy(
                src_ref=tok.at[own_tokens, pl.ds(pl.multiple_of(there * ROWS, ROWS), ROWS)],
                dst_ref=xt.at[me, y],
                send_sem=xsend.at[plane],
                recv_sem=xrecv.at[plane],
                device_id=where,
                device_id_type=MESH,
            ).start()

    exchange_tokens(0)
    weights.start_x(1)
    xt[me, y] = tok[own_tokens, pl.ds(pl.multiple_of(me * ROWS, ROWS), ROWS)]

    def share_of(k, plane):
        first = pl.multiple_of((1 - zh if plane else zh) * 8, 8)
        return xt.at[pl.ds(first, 8), lax.rem(y + k, 8)]

    def y_share(k, right, slot, plane):
        share = share_of(k, plane)
        pltpu.make_async_remote_copy(
            src_ref=share,
            dst_ref=share,
            send_sem=ysend,
            recv_sem=yrecv.at[plane * 7 + slot],
            device_id=y_at(1 if right else 7),
            device_id_type=MESH,
        ).start()

    def y_wait(k, slot, plane):
        wait_bytes(share_of(k, plane), yrecv.at[plane * 7 + slot])

    def y_first(plane):
        wait_bytes(xt.at[pl.ds(0, 7 + plane), 0], xrecv.at[plane])
        y_share(0, True, 0, plane)
        y_share(0, False, 4, plane)

    def y_step(s, plane):
        y_wait(8 - s, s - 1, plane)
        if s < 4:
            y_share(8 - s, True, s, plane)
        if s < 4:
            y_wait(s, 3 + s, plane)
        if s < 3:
            y_share(s, False, 4 + s, plane)

    def multiply(role, j):
        for k, (number, block) in enumerate(weights.blocks(role, j)):
            mine = tok[:, pl.ds(pl.multiple_of(number * ROWS, ROWS), ROWS)]
            product = lax.dot_general(
                block, mine, (((1,), (1,)), ((), ())), preferred_element_type=F32
            )
            acc[j] = product if role == "own" and k == 0 else acc[j] + product

    def activate(j):
        def some(i, carry):
            here = pl.ds(pl.multiple_of(j * CHUNK + i * 32, 32), 32)
            gate = acc[j, pl.ds(pl.multiple_of(i * 32, 32), 32), :]
            up = acc[j, pl.ds(pl.multiple_of(CHUNK + i * 32, 32), 32), :]
            back = cot[here, :].astype(F32)
            sig = jax.nn.sigmoid(gate)
            d_gate = back * up * sig * (1.0 + gate * (1.0 - sig))
            d_up = back * gate * sig
            hid[here, :] = (gate * sig * up).astype(BF16)
            for k, value in enumerate((d_gate, d_up)):
                there = pl.ds(
                    pl.multiple_of(own_row + k * COLS + j * CHUNK + i * 32, 32), 32
                )
                dbuf[there, :] = value.astype(BF16)
            return carry

        lax.fori_loop(0, CHUNK // 32, some, 0)

    deltas = Gather(at, dbuf, dtransit, dsend, drecv, drelay, dsib)

    def partial_inputs(k):
        pair = lax.rem(lax.rem(y + 4, 8) // 2 + k, 4)
        for run in range(4):
            product = jnp.dot(
                own[...], weights.block(run * 4 + pair), preferred_element_type=F32
            ).astype(BF16)
            term[pair * 2, run] = product[:, :128]
            term[pair * 2 + 1, run] = product[:, 128:]

    def target(d, s):
        return lax.rem(y + (4 - s if d == 0 else 4 + s), 8)

    def reduce_send(d, s, h):
        pltpu.make_async_remote_copy(
            src_ref=term.at[target(d, s), pl.ds(h * 2, 2)],
            dst_ref=landed.at[d, s, h],
            send_sem=rsend,
            recv_sem=rrecv.at[(d * 4 + s) * 2 + h],
            device_id=y_at(1 if d == 0 else 7),
            device_id_type=MESH,
        ).start()

    def reduce_wait(d, s, h):
        wait_bytes(landed.at[d, s, h], rrecv.at[(d * 4 + s) * 2 + h])

    def reduce_step(d, s, h):
        reduce_wait(d, s, h)
        goal = target(d, s + 1)

        def add(i, carry):
            here = pl.ds(pl.multiple_of(i * 64, 64), 64)
            for k in range(2):
                came = landed[d, s, h, k, here].astype(F32)
                mine = term[goal, h * 2 + k, here].astype(F32)
                term[goal, h * 2 + k, here] = (mine + came).astype(BF16)
            return carry

        lax.fori_loop(0, ROWS // 64, add, 0)
        reduce_send(d, s + 1, h)

    def reduce_last():
        for h in range(2):
            for d in range(2):
                reduce_wait(d, 3, h)
        for k in (1, 2, 3, 0):
            run = lax.rem(zl + k, 4)

            def add(i, carry, k=k, run=run):
                here = pl.ds(pl.multiple_of(i * 64, 64), 64)
                total = term[y, run, here].astype(F32)
                for d in range(2):
                    total = total + landed[d, 3, run // 2, lax.rem(run, 2), here].astype(F32)
                if k:
                    zsend[k - 1, here] = total.astype(BF16)
                else:
                    igacc[here] = total
                return carry

            lax.fori_loop(0, ROWS // 64, add, 0)
            if k:
                pltpu.make_async_remote_copy(
                    src_ref=zsend.at[k - 1],
                    dst_ref=zland.at[k - 1],
                    send_sem=zs_send,
                    recv_sem=zs_recv,
                    device_id={"outer_0": run},
                    device_id_type=MESH,
                ).start()

    def input_done():
        wait_bytes(zland, zs_recv)

        def add(i, carry):
            here = pl.ds(pl.multiple_of(i * 64, 64), 64)
            total = igacc[here]
            for k in range(3):
                total = total + zland[k, here].astype(F32)
            ig[here] = total.astype(BF16)
            return carry

        lax.fori_loop(0, ROWS // 64, add, 0)

    def accumulate(role, j):
        for k, (number, block) in enumerate(deltas.blocks(role, j)):
            product = jnp.dot(
                block, xt[number].reshape(ROWS, ROWS), preferred_element_type=F32
            )
            acc[j] = product if role == "own" and k == 0 else acc[j] + product

    def totals(j, squares):
        def some(i, squares):
            here = pl.ds(pl.multiple_of(j * CHUNK + i * 32, 32), 32)
            for k in range(2):
                grad = acc[j, pl.ds(pl.multiple_of(k * CHUNK + i * 32, 32), 32), :]
                total = scaled(gc, k, here) + grad
                upd[k, here, :] = total
                squares = squares + jnp.sum((total * total).reshape(4, 8, ROWS), axis=0)
            return squares

        return lax.fori_loop(0, CHUNK // 32, some, squares)

    multiply("own", 0)
    weights.first_hop(0)
    multiply("own", 1)
    weights.pass_on(0)
    weights.near_done(0)
    weights.pass_on(1)
    weights.first_hop(1)
    weights.pass_on(2)
    weights.near_done(1)
    weights.pass_on(3)
    multiply("r", 0)
    multiply("l", 0)
    y_first(0)
    weights.far_done(0)
    weights.partner(0)
    multiply("r", 1)
    multiply("l", 1)
    weights.far_done(1)
    weights.partner(1)
    y_step(1, 0)
    multiply("a", 0)
    weights.partner_hop(0)
    weights.partner(2)
    exchange_tokens(1)
    multiply("a", 1)
    weights.partner_hop(1)
    weights.partner(3)
    y_step(2, 0)
    multiply("p", 0)
    weights.partner_near_done(0)
    multiply("pl", 0)
    multiply("pr", 0)
    weights.partner_hop(2)
    weights.partner_far_done(0)
    y_step(3, 0)
    loads[3].wait()
    multiply("pa", 0)
    activate(0)
    deltas.start_z((0, 1))
    deltas.start_x(0)
    y_first(1)
    weights.partner_hop(3)
    multiply("p", 1)
    weights.partner_near_done(1)
    y_step(4, 0)
    multiply("pl", 1)
    multiply("pr", 1)
    deltas.pass_on(0)
    deltas.first_hop(0)
    deltas.pass_on(1)
    weights.partner_far_done(1)
    y_step(1, 1)
    multiply("pa", 1)
    activate(1)
    deltas.start_z((2, 3))
    deltas.start_x(1)

    for t in range(CAT // 128):
        there = pl.ds(pl.multiple_of(own_row + t * 128, 128), 128)
        own[:, t * 128 : (t + 1) * 128] = jnp.transpose(dbuf[there, :])
    partial_inputs(0)
    reduce_send(0, 0, 0)
    reduce_send(1, 0, 1)
    deltas.near_done(0)
    partial_inputs(1)
    partial_inputs(3)
    reduce_send(0, 1, 1)
    reduce_send(1, 1, 0)
    deltas.far_done(0)
    deltas.partner(0)
    partial_inputs(2)
    y_step(2, 1)
    deltas.first_hop(1)
    deltas.pass_on(2)
    deltas.partner(1)
    reduce_step(0, 0, 0)
    reduce_step(1, 0, 1)
    deltas.near_done(1)
    deltas.pass_on(3)
    accumulate("own", 0)
    accumulate("r", 0)
    accumulate("l", 0)
    deltas.partner_hop(0)
    reduce_step(0, 1, 1)
    reduce_step(1, 1, 0)
    y_step(3, 1)
    deltas.far_done(1)
    deltas.partner_hop(1)
    deltas.partner(2)
    reduce_step(0, 1, 0)
    reduce_step(1, 1, 1)
    accumulate("own", 1)
    accumulate("a", 0)
    deltas.partner(3)
    deltas.partner_near_done(0)
    accumulate("r", 1)
    accumulate("l", 1)
    deltas.partner_hop(2)
    reduce_step(0, 2, 1)
    reduce_step(1, 2, 0)
    deltas.partner_far_done(0)
    y_step(4, 1)
    accumulate("a", 1)
    accumulate("p", 0)
    deltas.partner_hop(3)
    accumulate("pl", 0)
    accumulate("pr", 0)
    reduce_step(0, 2, 0)
    reduce_step(1, 2, 1)
    accumulate("pa", 0)
    accumulate("p", 1)
    deltas.partner_near_done(1)
    loads[4].wait()
    loads[5].wait()
    columns(gs)
    squares = totals(0, jnp.zeros((8, ROWS), F32))
    accumulate("pl", 1)
    accumulate("pr", 1)
    deltas.partner_far_done(1)
    accumulate("pa", 1)
    squares = totals(1, squares)
    part[0] = jnp.broadcast_to(jnp.sum(squares, keepdims=True), (8, 128))
    value = part[0]
    for stage, peer in enumerate((plane_at, z_at, y_at)):
        for k in range(1, 8):
            pltpu.make_async_remote_copy(
                src_ref=part.at[stage],
                dst_ref=parts.at[stage, k - 1],
                send_sem=msend.at[stage],
                recv_sem=mrecv.at[stage],
                device_id=peer(k),
                device_id_type=MESH,
            ).start()
        if stage == 0:
            reduce_last()
        wait_bytes(parts.at[stage], mrecv.at[stage])
        for k in range(7):
            value = value + parts[stage, k]
        if stage < 2:
            part[stage + 1] = value
    input_done()
    scale[...] = 1.0 / jnp.sqrt(value / (2.0 * D * FF) + 1e-06)

    weights.finish()
    deltas.finish()
    for plane in range(2):
        wait_bytes(xt.at[pl.ds(0, 7 + plane), 0], xsend.at[plane])
    wait_bytes(xt.at[:, pl.ds(0, 7)], ysend)
    wait_bytes(term.at[pl.ds(0, 7)], rsend)
    wait_bytes(zsend, zs_send)
    for stage in range(3):
        wait_bytes(parts.at[stage], msend.at[stage])

def finish(hid, ig, total, scale, hid_o, ig_o, upd_o, upd, sem):
    outs = [pltpu.make_async_copy(hid, hid_o, sem.at[0]), pltpu.make_async_copy(ig, ig_o, sem.at[1])]
    for out in outs:
        out.start()
    factor = scale[0:1, 0:1]
    for half in range(2):

        def normalize(i, carry, half=half):
            here = pl.ds(pl.multiple_of(i * 64, 64), 64)
            upd[half, here, :] = total[half, here, :] * factor
            return carry

        lax.fori_loop(0, COLS // 64, normalize, 0)
        out = pltpu.make_async_copy(upd.at[half], upd_o.at[half], sem.at[2 + half])
        out.start()
        outs.append(out)
    for out in outs:
        out.wait()


def local(tokens, weight_codes, weight_scales, grad_codes, grad_scales, cotangent):
    dma = pltpu.SemaphoreType.DMA
    slots = len(GATHER_SLOTS)
    gather = [dma, dma((slots,)), dma((8,)), dma((32,))]
    call = pl.pallas_call(
        kernel,
        out_shape=(
            pltpu.VMEM((COLS, ROWS), BF16),
            pltpu.VMEM((ROWS, 128), BF16),
            pltpu.VMEM((2, COLS, ROWS), F32),
            pltpu.VMEM((8, 128), F32),
        ),
        in_specs=[pl.BlockSpec(memory_space=pltpu.HBM)] * 6,
        out_specs=[pl.BlockSpec(memory_space=pltpu.VMEM)] * 4,
        scratch_shapes=[
            pltpu.VMEM((ROWS, D), BF16),
            pltpu.VMEM((2, COLS, ROWS), jnp.int32),
            pltpu.VMEM((2, 2, COLS), F32),
            pltpu.VMEM((2, COLS, ROWS), jnp.int32),
            pltpu.VMEM((2, 2, COLS), F32),
            pltpu.VMEM((COLS, ROWS), BF16),
            pltpu.VMEM((16 * CAT, ROWS), BF16),
            pltpu.VMEM((16 * CAT, ROWS), BF16),
            pltpu.VMEM((8, PIECE, ROWS), BF16),
            pltpu.VMEM((8, PIECE, ROWS), BF16),
            pltpu.VMEM((16, 8, 32, ROWS), BF16),
            pltpu.VMEM((2, COLS, ROWS), F32),
            pltpu.VMEM((8, 4, ROWS, 128), BF16),
            pltpu.VMEM((2, 4, 2, 2, ROWS, 128), BF16),
            pltpu.VMEM((3, ROWS, 128), BF16),
            pltpu.VMEM((3, ROWS, 128), BF16),
            pltpu.VMEM((ROWS, 128), F32),
            pltpu.VMEM((ROWS, CAT), BF16),
            pltpu.VMEM((8, 512), F32),
            pltpu.VMEM((512, 8), F32),
            pltpu.VMEM((3, 8, 128), F32),
            pltpu.VMEM((3, 7, 8, 128), F32),
            dma((6,)),
            *gather,
            *gather,
            dma((2,)),
            dma((2,)),
            dma,
            dma((14,)),
            dma,
            dma((16,)),
            dma,
            dma,
            dma((3,)),
            dma((3,)),
        ],
        compiler_params=pltpu.CompilerParams(
            collective_id=0, has_side_effects=True, vmem_limit_bytes=48 * 1024 * 1024
        ),
    )
    given = (
        tokens,
        weight_codes.transpose(0, 2, 1),
        weight_scales,
        grad_codes.transpose(0, 2, 1),
        grad_scales,
        cotangent.T,
    )
    made = call(*(pltpu.with_memory_space_constraint(a, pltpu.HBM) for a in given))
    hidden, input_grad, update = pl.pallas_call(
        finish,
        out_shape=(
            jax.ShapeDtypeStruct((COLS, ROWS), BF16),
            jax.ShapeDtypeStruct((ROWS, 128), BF16),
            jax.ShapeDtypeStruct((2, COLS, ROWS), F32),
        ),
        in_specs=[pl.BlockSpec(memory_space=pltpu.VMEM)] * 4,
        out_specs=[pl.BlockSpec(memory_space=pltpu.HBM)] * 3,
        scratch_shapes=[pltpu.VMEM((2, COLS, ROWS), F32), dma((4,))],
        compiler_params=pltpu.CompilerParams(vmem_limit_bytes=8 * 1024 * 1024),
    )(*made)
    return hidden.T, input_grad, update.transpose(0, 2, 1)


def solution(mesh):
    finer = Mesh(
        mesh.devices.reshape(4, 8, 2, 4, 2), ("outer_0", "outer_1", "inner_0", "inner_1", "inner_2")
    )
    return jax.shard_map(
        local,
        mesh=finer,
        in_specs=(
            P(INNER, None),
            P(None, INNER, OUTER),
            P(None, INNER, OUTER),
            P(None, INNER, OUTER),
            P(None, INNER, OUTER),
            P(INNER, OUTER),
        ),
        out_specs=(P(INNER, OUTER), P(INNER, OUTER), P(None, INNER, OUTER)),
        check_vma=False,
    )
```

```python
import jax
import jax.numpy as jnp
from jax import lax
from jax.experimental import pallas as pl
from jax.experimental.pallas import tpu as pltpu
from jax.sharding import Mesh
from jax.sharding import PartitionSpec as P

D = 4096
FF = 14336
QBLOCK = 128
INNER = ("inner_0", "inner_1", "inner_2")
OUTER = ("outer_0", "outer_1")
ROWS = 256
COLS = 448
CAT = 2 * COLS
MESH = pl.DeviceIdType.MESH
F32 = jnp.float32
BF16 = jnp.bfloat16

CHUNK = COLS // 2
PIECE = COLS // 4

GATHER_SLOTS = {
    name: k
    for k, name in enumerate(
        [f"{b}{g}{j}" for b in ("l", "r", "a") for g in range(2) for j in range(2)]
        + [f"{b}{q}" for b in ("p", "pl", "pr", "pa") for q in range(8)]
    )
}
ROLES = ("own", "r", "l", "a", "p", "pr", "pl", "pa")


def wait_bytes(ref, sem):
    pltpu.make_async_copy(ref, ref, sem).wait()


class Gather:
    def __init__(self, at, buf, transit, send, recv, relay, sib):
        self.at, self.buf, self.transit = at, buf, transit
        self.send, self.recv, self.relay, self.sib = send, recv, relay, sib
        zh, x, c = at["zh"], at["x"], at["c"]

        def chip(h, k):
            return h * 4 + lax.rem(x + k, 4)

        other = 1 - zh
        self.chip = {
            "own": chip(zh, 0),
            "r": chip(zh, 1),
            "a": chip(zh, 2),
            "l": chip(zh, 3),
            "p": chip(other, 0),
            "pr": chip(other, 1),
            "pa": chip(other, 2),
            "pl": chip(other, 3),
        }

    def rows(self, role, first, count, sibling=False):
        c = self.at["c"]
        block = self.chip[role] * 2 + (1 - c if sibling else c)
        return self.buf.at[pl.ds(pl.multiple_of(block * CAT + first, 16), count)]

    def piece(self, role, q):
        return self.rows(role, q * PIECE, PIECE)

    def copy(self, src, dst, recv, where):
        pltpu.make_async_remote_copy(
            src_ref=src,
            dst_ref=dst,
            send_sem=self.send,
            recv_sem=recv,
            device_id=where,
            device_id_type=MESH,
        ).start()

    def along_x(self, part, right, slot):
        where = {"inner_1": self.at["right"] if right else self.at["left"]}
        self.copy(part, part, self.recv.at[GATHER_SLOTS[slot]], where)

    def part(self, role, g, j, sibling=False):
        return self.rows(role, g * COLS + j * CHUNK, CHUNK, sibling)

    def along_z(self, q):
        where = self.at["up2"] if q < 4 else self.at["down2"]
        self.copy(self.piece("own", q), self.transit.at[q], self.relay.at[q], where)

    def pass_on(self, k):
        at = self.at
        for q in (k, k + 4):
            wait_bytes(self.transit.at[q], self.relay.at[q])
            origin = at["down2"] if q < 4 else at["up2"]
            where = at["up2"] if q < 4 else at["down2"]
            block = (origin["inner_0"] * 4 + at["x"]) * 2 + at["c"]
            dst = self.buf.at[pl.ds(pl.multiple_of(block * CAT + q * PIECE, 16), PIECE)]
            self.copy(self.transit.at[q], dst, self.recv.at[GATHER_SLOTS[f"p{q}"]], where)

    def sibling_sem(self, role, g, j):
        return self.sib.at[(ROLES.index(role) * 2 + j) * 2 + g]

    def to_sibling(self, role, j):
        for g in range(2):
            part = self.part(role, g, j)
            self.copy(part, part, self.sibling_sem(role, g, j), {"inner_2": 1 - self.at["c"]})

    def start_z(self, ks):
        for k in ks:
            self.along_z(k)
            self.along_z(k + 4)

    def start_x(self, j):
        self.along_x(self.part("own", 0, j), True, f"l0{j}")
        self.along_x(self.part("own", 1, j), False, f"r1{j}")
        self.along_x(self.part("own", 1, j), True, f"l1{j}")
        self.along_x(self.part("own", 0, j), False, f"r0{j}")
        self.to_sibling("own", j)

    def wait_part(self, role, g, j):
        wait_bytes(self.part(role, g, j), self.recv.at[GATHER_SLOTS[f"{role}{g}{j}"]])

    def wait_piece(self, role, q):
        wait_bytes(self.piece(role, q), self.recv.at[GATHER_SLOTS[f"{role}{q}"]])

    def first_hop(self, j):
        self.wait_part("l", 0, j)
        self.along_x(self.part("l", 0, j), True, f"a0{j}")
        self.wait_part("r", 1, j)
        self.along_x(self.part("r", 1, j), False, f"a1{j}")

    def near_done(self, j):
        self.wait_part("l", 1, j)
        self.to_sibling("l", j)
        self.wait_part("r", 0, j)
        self.to_sibling("r", j)

    def far_done(self, j):
        self.wait_part("a", 0, j)
        self.wait_part("a", 1, j)
        self.to_sibling("a", j)

    def partner(self, k):
        for q in (k, k + 4):
            self.wait_piece("p", q)
            self.along_x(self.piece("p", q), True, f"pl{q}")
            self.along_x(self.piece("p", q), False, f"pr{q}")
        if k % 2 == 1:
            self.to_sibling("p", k // 2)

    def partner_hop(self, k):
        self.wait_piece("pl", k)
        self.along_x(self.piece("pl", k), True, f"pa{k}")
        self.wait_piece("pr", k + 4)
        self.along_x(self.piece("pr", k + 4), False, f"pa{k + 4}")

    def partner_near_done(self, j):
        for q in (4 + 2 * j, 5 + 2 * j):
            self.wait_piece("pl", q)
        self.to_sibling("pl", j)
        for q in (2 * j, 2 * j + 1):
            self.wait_piece("pr", q)
        self.to_sibling("pr", j)

    def partner_far_done(self, j):
        for k in (2 * j, 2 * j + 1):
            self.wait_piece("pa", k)
            self.wait_piece("pa", k + 4)
        self.to_sibling("pa", j)

    def blocks(self, role, j):
        c = self.at["c"]
        for k, which in enumerate((c, 1 - c)):
            parts = [self.part(role, g, j, k == 1) for g in range(2)]
            if k:
                for g in range(2):
                    wait_bytes(parts[g], self.sibling_sem(role, g, j))
            yield self.chip[role] * 2 + which, jnp.concatenate([p[...] for p in parts], axis=0)

    def block(self, number):
        return self.buf[pl.ds(pl.multiple_of(number * CAT, CAT), CAT), :]

    def finish(self):
        wait_bytes(self.buf, self.send)


def kernel(
    tok_h,
    wc_h,
    ws_h,
    gc_h,
    gs_h,
    cot_h,
    hid,
    ig,
    upd,
    scale,
    tok,
    wc,
    ws,
    gc,
    gs,
    cot,
    wbuf,
    dbuf,
    wtransit,
    dtransit,
    xt,
    acc,
    term,
    landed,
    zsend,
    zland,
    igacc,
    own,
    lanes,
    column,
    part,
    parts,
    load_sem,
    wsend,
    wrecv,
    wrelay,
    wsib,
    dsend,
    drecv,
    drelay,
    dsib,
    xsend,
    xrecv,
    ysend,
    yrecv,
    rsend,
    rrecv,
    zs_send,
    zs_recv,
    msend,
    mrecv,
):
    zl, y = lax.axis_index("outer_0"), lax.axis_index("outer_1")
    zh, x, c = (lax.axis_index(a) for a in INNER)
    z = zh * 4 + zl
    me = (zh * 4 + x) * 2 + c

    def z_at(k):
        there = lax.rem(z + k, 8)
        return {"outer_0": lax.rem(there, 4), "inner_0": there // 4}

    def plane_at(k):
        there = lax.rem(x * 2 + c + k, 8)
        return {"inner_1": there // 2, "inner_2": lax.rem(there, 2)}

    def y_at(k):
        return {"outer_1": lax.rem(y + k, 8)}

    at = {
        "zh": zh,
        "x": x,
        "c": c,
        "right": lax.rem(x + 1, 4),
        "left": lax.rem(x + 3, 4),
        "up2": z_at(2),
        "down2": z_at(6),
    }

    loads = [
        pltpu.make_async_copy(src, dst, load_sem.at[k])
        for k, (src, dst) in enumerate(
            ((ws_h, ws), (wc_h, wc), (tok_h, tok), (cot_h, cot), (gs_h, gs), (gc_h, gc))
        )
    ]
    for load in loads[:2]:
        load.start()

    barrier = pltpu.get_barrier_semaphore()
    greeted = [plane_at(k) for k in range(1, 8)]
    greeted += [z_at(k) for k in (1, 2, 6, 7)]
    greeted += [y_at(k) for k in (1, 7)]
    for where in greeted:
        pl.semaphore_signal(barrier, inc=1, device_id=where, device_id_type=MESH)

    for load in loads[2:]:
        load.start()

    loads[0].wait()
    loads[1].wait()
    own_row = pl.multiple_of(me * CAT, CAT)

    def columns(scales):
        for k in range(2):
            for g in range(2):
                lanes[2 * k + g : 2 * k + g + 1, 0:COLS] = scales[k, g : g + 1, :]
        column[...] = jnp.transpose(lanes[...])

    def scaled(codes, k, here):
        parts = [
            codes[k, here, g * QBLOCK : (g + 1) * QBLOCK].astype(F32)
            * column[here, 2 * k + g : 2 * k + g + 1]
            for g in range(2)
        ]
        return jnp.concatenate(parts, axis=1)

    columns(ws)

    def dequantize(first):
        def some(i, carry):
            here = pl.ds(pl.multiple_of(first * 32 + i * 32, 32), 32)
            for k in range(2):
                there = pl.ds(pl.multiple_of(own_row + k * COLS + first * 32 + i * 32, 32), 32)
                wbuf[there, :] = scaled(wc, k, here).astype(BF16)
            return carry

        lax.fori_loop(0, COLS // 64, some, 0)

    weights = Gather(at, wbuf, wtransit, wsend, wrecv, wrelay, wsib)
    dequantize(0)
    pl.semaphore_wait(barrier, len(greeted))
    weights.start_z((0, 1))
    weights.start_x(0)
    dequantize(COLS // 64)
    weights.start_z((2, 3))
    loads[2].wait()

    own_tokens = pl.ds(pl.multiple_of(y * 32, 32), 32)

    def exchange_tokens(plane):
        for k in range(0 if plane else 1, 8):
            spot = lax.rem(x * 2 + c + k, 8)
            there = (1 - zh if plane else zh) * 8 + spot
            where = {
                "inner_0": there // 8,
                "inner_1": lax.rem(there // 2, 4),
                "inner_2": lax.rem(there, 2),
            }
            pltpu.make_async_remote_copy(
                src_ref=tok.at[own_tokens, pl.ds(pl.multiple_of(there * ROWS, ROWS), ROWS)],
                dst_ref=xt.at[me, y],
                send_sem=xsend.at[plane],
                recv_sem=xrecv.at[plane],
                device_id=where,
                device_id_type=MESH,
            ).start()

    exchange_tokens(0)
    weights.start_x(1)
    xt[me, y] = tok[own_tokens, pl.ds(pl.multiple_of(me * ROWS, ROWS), ROWS)]

    def share_of(k, plane):
        first = pl.multiple_of((1 - zh if plane else zh) * 8, 8)
        return xt.at[pl.ds(first, 8), lax.rem(y + k, 8)]

    def y_share(k, right, slot, plane):
        share = share_of(k, plane)
        pltpu.make_async_remote_copy(
            src_ref=share,
            dst_ref=share,
            send_sem=ysend,
            recv_sem=yrecv.at[plane * 7 + slot],
            device_id=y_at(1 if right else 7),
            device_id_type=MESH,
        ).start()

    def y_wait(k, slot, plane):
        wait_bytes(share_of(k, plane), yrecv.at[plane * 7 + slot])

    def y_first(plane):
        wait_bytes(xt.at[pl.ds(0, 7 + plane), 0], xrecv.at[plane])
        y_share(0, True, 0, plane)
        y_share(0, False, 4, plane)

    def y_step(s, plane):
        y_wait(8 - s, s - 1, plane)
        if s < 4:
            y_share(8 - s, True, s, plane)
        if s < 4:
            y_wait(s, 3 + s, plane)
        if s < 3:
            y_share(s, False, 4 + s, plane)

    def multiply(role, j):
        for k, (number, block) in enumerate(weights.blocks(role, j)):
            mine = tok[:, pl.ds(pl.multiple_of(number * ROWS, ROWS), ROWS)]
            product = lax.dot_general(
                block, mine, (((1,), (1,)), ((), ())), preferred_element_type=F32
            )
            acc[j] = product if role == "own" and k == 0 else acc[j] + product

    def activate(j):
        def some(i, carry):
            here = pl.ds(pl.multiple_of(j * CHUNK + i * 32, 32), 32)
            gate = acc[j, pl.ds(pl.multiple_of(i * 32, 32), 32), :]
            up = acc[j, pl.ds(pl.multiple_of(CHUNK + i * 32, 32), 32), :]
            back = cot[here, :].astype(F32)
            sig = jax.nn.sigmoid(gate)
            d_gate = back * up * sig * (1.0 + gate * (1.0 - sig))
            d_up = back * gate * sig
            hid[here, :] = (gate * sig * up).astype(BF16)
            for k, value in enumerate((d_gate, d_up)):
                there = pl.ds(
                    pl.multiple_of(own_row + k * COLS + j * CHUNK + i * 32, 32), 32
                )
                dbuf[there, :] = value.astype(BF16)
            return carry

        lax.fori_loop(0, CHUNK // 32, some, 0)

    deltas = Gather(at, dbuf, dtransit, dsend, drecv, drelay, dsib)

    def partial_inputs(k):
        pair = lax.rem(lax.rem(y + 4, 8) // 2 + k, 4)
        for run in range(4):
            product = jnp.dot(
                own[...], weights.block(run * 4 + pair), preferred_element_type=F32
            ).astype(BF16)
            term[pair * 2, run] = product[:, :128]
            term[pair * 2 + 1, run] = product[:, 128:]

    def target(d, s):
        return lax.rem(y + (4 - s if d == 0 else 4 + s), 8)

    def reduce_send(d, s, h):
        pltpu.make_async_remote_copy(
            src_ref=term.at[target(d, s), pl.ds(h * 2, 2)],
            dst_ref=landed.at[d, s, h],
            send_sem=rsend,
            recv_sem=rrecv.at[(d * 4 + s) * 2 + h],
            device_id=y_at(1 if d == 0 else 7),
            device_id_type=MESH,
        ).start()

    def reduce_wait(d, s, h):
        wait_bytes(landed.at[d, s, h], rrecv.at[(d * 4 + s) * 2 + h])

    def reduce_step(d, s, h):
        reduce_wait(d, s, h)
        goal = target(d, s + 1)

        def add(i, carry):
            here = pl.ds(pl.multiple_of(i * 64, 64), 64)
            for k in range(2):
                came = landed[d, s, h, k, here].astype(F32)
                mine = term[goal, h * 2 + k, here].astype(F32)
                term[goal, h * 2 + k, here] = (mine + came).astype(BF16)
            return carry

        lax.fori_loop(0, ROWS // 64, add, 0)
        reduce_send(d, s + 1, h)

    def reduce_last():
        for h in range(2):
            for d in range(2):
                reduce_wait(d, 3, h)
        for k in (1, 2, 3, 0):
            run = lax.rem(zl + k, 4)

            def add(i, carry, k=k, run=run):
                here = pl.ds(pl.multiple_of(i * 64, 64), 64)
                total = term[y, run, here].astype(F32)
                for d in range(2):
                    total = total + landed[d, 3, run // 2, lax.rem(run, 2), here].astype(F32)
                if k:
                    zsend[k - 1, here] = total.astype(BF16)
                else:
                    igacc[here] = total
                return carry

            lax.fori_loop(0, ROWS // 64, add, 0)
            if k:
                pltpu.make_async_remote_copy(
                    src_ref=zsend.at[k - 1],
                    dst_ref=zland.at[k - 1],
                    send_sem=zs_send,
                    recv_sem=zs_recv,
                    device_id={"outer_0": run},
                    device_id_type=MESH,
                ).start()

    def input_done():
        wait_bytes(zland, zs_recv)

        def add(i, carry):
            here = pl.ds(pl.multiple_of(i * 64, 64), 64)
            total = igacc[here]
            for k in range(3):
                total = total + zland[k, here].astype(F32)
            ig[here] = total.astype(BF16)
            return carry

        lax.fori_loop(0, ROWS // 64, add, 0)

    def accumulate(role, j):
        for k, (number, block) in enumerate(deltas.blocks(role, j)):
            product = jnp.dot(
                block, xt[number].reshape(ROWS, ROWS), preferred_element_type=F32
            )
            acc[j] = product if role == "own" and k == 0 else acc[j] + product

    def totals(j, squares):
        def some(i, squares):
            here = pl.ds(pl.multiple_of(j * CHUNK + i * 32, 32), 32)
            for k in range(2):
                grad = acc[j, pl.ds(pl.multiple_of(k * CHUNK + i * 32, 32), 32), :]
                total = scaled(gc, k, here) + grad
                upd[k, here, :] = total
                squares = squares + jnp.sum((total * total).reshape(4, 8, ROWS), axis=0)
            return squares

        return lax.fori_loop(0, CHUNK // 32, some, squares)

    multiply("own", 0)
    weights.first_hop(0)
    multiply("own", 1)
    weights.pass_on(0)
    weights.near_done(0)
    weights.pass_on(1)
    weights.first_hop(1)
    weights.pass_on(2)
    weights.near_done(1)
    weights.pass_on(3)
    multiply("r", 0)
    multiply("l", 0)
    y_first(0)
    weights.far_done(0)
    weights.partner(0)
    multiply("r", 1)
    multiply("l", 1)
    weights.far_done(1)
    weights.partner(1)
    y_step(1, 0)
    multiply("a", 0)
    weights.partner_hop(0)
    weights.partner(2)
    exchange_tokens(1)
    multiply("a", 1)
    weights.partner_hop(1)
    weights.partner(3)
    y_step(2, 0)
    multiply("p", 0)
    weights.partner_near_done(0)
    multiply("pl", 0)
    multiply("pr", 0)
    weights.partner_hop(2)
    weights.partner_far_done(0)
    y_step(3, 0)
    loads[3].wait()
    multiply("pa", 0)
    activate(0)
    deltas.start_z((0, 1))
    deltas.start_x(0)
    y_first(1)
    weights.partner_hop(3)
    multiply("p", 1)
    weights.partner_near_done(1)
    y_step(4, 0)
    multiply("pl", 1)
    multiply("pr", 1)
    deltas.pass_on(0)
    deltas.first_hop(0)
    deltas.pass_on(1)
    weights.partner_far_done(1)
    y_step(1, 1)
    multiply("pa", 1)
    activate(1)
    deltas.start_z((2, 3))
    deltas.start_x(1)

    for t in range(CAT // 128):
        there = pl.ds(pl.multiple_of(own_row + t * 128, 128), 128)
        own[:, t * 128 : (t + 1) * 128] = jnp.transpose(dbuf[there, :])
    partial_inputs(0)
    reduce_send(0, 0, 0)
    reduce_send(1, 0, 1)
    deltas.near_done(0)
    partial_inputs(1)
    partial_inputs(3)
    reduce_send(0, 1, 1)
    reduce_send(1, 1, 0)
    deltas.far_done(0)
    deltas.partner(0)
    partial_inputs(2)
    y_step(2, 1)
    deltas.first_hop(1)
    deltas.pass_on(2)
    deltas.partner(1)
    reduce_step(0, 0, 0)
    reduce_step(1, 0, 1)
    deltas.near_done(1)
    deltas.pass_on(3)
    accumulate("own", 0)
    accumulate("r", 0)
    accumulate("l", 0)
    deltas.partner_hop(0)
    reduce_step(0, 1, 1)
    reduce_step(1, 1, 0)
    deltas.partner(2)
    deltas.far_done(1)
    deltas.partner_hop(1)
    reduce_step(0, 1, 0)
    reduce_step(1, 1, 1)
    deltas.partner(3)
    y_step(3, 1)
    accumulate("own", 1)
    accumulate("a", 0)
    deltas.partner_near_done(0)
    accumulate("r", 1)
    accumulate("l", 1)
    deltas.partner_hop(2)
    reduce_step(0, 2, 1)
    reduce_step(1, 2, 0)
    deltas.partner_far_done(0)
    accumulate("a", 1)
    deltas.partner_hop(3)
    y_step(4, 1)
    accumulate("p", 0)
    accumulate("pl", 0)
    accumulate("pr", 0)
    reduce_step(0, 2, 0)
    reduce_step(1, 2, 1)
    accumulate("pa", 0)
    accumulate("p", 1)
    deltas.partner_near_done(1)
    loads[4].wait()
    loads[5].wait()
    columns(gs)
    squares = totals(0, jnp.zeros((8, ROWS), F32))
    accumulate("pl", 1)
    accumulate("pr", 1)
    deltas.partner_far_done(1)
    accumulate("pa", 1)
    squares = totals(1, squares)
    part[0] = jnp.broadcast_to(jnp.sum(squares, keepdims=True), (8, 128))
    value = part[0]
    for stage, peer in enumerate((plane_at, z_at, y_at)):
        for k in range(1, 8):
            pltpu.make_async_remote_copy(
                src_ref=part.at[stage],
                dst_ref=parts.at[stage, k - 1],
                send_sem=msend.at[stage],
                recv_sem=mrecv.at[stage],
                device_id=peer(k),
                device_id_type=MESH,
            ).start()
        if stage == 0:
            reduce_last()
        wait_bytes(parts.at[stage], mrecv.at[stage])
        for k in range(7):
            value = value + parts[stage, k]
        if stage < 2:
            part[stage + 1] = value
    input_done()
    scale[...] = 1.0 / jnp.sqrt(value / (2.0 * D * FF) + 1e-06)

    weights.finish()
    deltas.finish()
    for plane in range(2):
        wait_bytes(xt.at[pl.ds(0, 7 + plane), 0], xsend.at[plane])
    wait_bytes(xt.at[:, pl.ds(0, 7)], ysend)
    wait_bytes(term.at[pl.ds(0, 7)], rsend)
    wait_bytes(zsend, zs_send)
    for stage in range(3):
        wait_bytes(parts.at[stage], msend.at[stage])

def finish(hid, ig, total, scale, hid_o, ig_o, upd_o, upd, sem):
    outs = [pltpu.make_async_copy(hid, hid_o, sem.at[0]), pltpu.make_async_copy(ig, ig_o, sem.at[1])]
    for out in outs:
        out.start()
    factor = scale[0:1, 0:1]
    for half in range(2):

        def normalize(i, carry, half=half):
            here = pl.ds(pl.multiple_of(i * 64, 64), 64)
            upd[half, here, :] = total[half, here, :] * factor
            return carry

        lax.fori_loop(0, COLS // 64, normalize, 0)
        out = pltpu.make_async_copy(upd.at[half], upd_o.at[half], sem.at[2 + half])
        out.start()
        outs.append(out)
    for out in outs:
        out.wait()


def local(tokens, weight_codes, weight_scales, grad_codes, grad_scales, cotangent):
    dma = pltpu.SemaphoreType.DMA
    slots = len(GATHER_SLOTS)
    gather = [dma, dma((slots,)), dma((8,)), dma((32,))]
    call = pl.pallas_call(
        kernel,
        out_shape=(
            pltpu.VMEM((COLS, ROWS), BF16),
            pltpu.VMEM((ROWS, 128), BF16),
            pltpu.VMEM((2, COLS, ROWS), F32),
            pltpu.VMEM((8, 128), F32),
        ),
        in_specs=[pl.BlockSpec(memory_space=pltpu.HBM)] * 6,
        out_specs=[pl.BlockSpec(memory_space=pltpu.VMEM)] * 4,
        scratch_shapes=[
            pltpu.VMEM((ROWS, D), BF16),
            pltpu.VMEM((2, COLS, ROWS), jnp.int32),
            pltpu.VMEM((2, 2, COLS), F32),
            pltpu.VMEM((2, COLS, ROWS), jnp.int32),
            pltpu.VMEM((2, 2, COLS), F32),
            pltpu.VMEM((COLS, ROWS), BF16),
            pltpu.VMEM((16 * CAT, ROWS), BF16),
            pltpu.VMEM((16 * CAT, ROWS), BF16),
            pltpu.VMEM((8, PIECE, ROWS), BF16),
            pltpu.VMEM((8, PIECE, ROWS), BF16),
            pltpu.VMEM((16, 8, 32, ROWS), BF16),
            pltpu.VMEM((2, COLS, ROWS), F32),
            pltpu.VMEM((8, 4, ROWS, 128), BF16),
            pltpu.VMEM((2, 4, 2, 2, ROWS, 128), BF16),
            pltpu.VMEM((3, ROWS, 128), BF16),
            pltpu.VMEM((3, ROWS, 128), BF16),
            pltpu.VMEM((ROWS, 128), F32),
            pltpu.VMEM((ROWS, CAT), BF16),
            pltpu.VMEM((8, 512), F32),
            pltpu.VMEM((512, 8), F32),
            pltpu.VMEM((3, 8, 128), F32),
            pltpu.VMEM((3, 7, 8, 128), F32),
            dma((6,)),
            *gather,
            *gather,
            dma((2,)),
            dma((2,)),
            dma,
            dma((14,)),
            dma,
            dma((16,)),
            dma,
            dma,
            dma((3,)),
            dma((3,)),
        ],
        compiler_params=pltpu.CompilerParams(
            collective_id=0, has_side_effects=True, vmem_limit_bytes=48 * 1024 * 1024
        ),
    )
    given = (
        tokens,
        weight_codes.transpose(0, 2, 1),
        weight_scales,
        grad_codes.transpose(0, 2, 1),
        grad_scales,
        cotangent.T,
    )
    made = call(*(pltpu.with_memory_space_constraint(a, pltpu.HBM) for a in given))
    hidden, input_grad, update = pl.pallas_call(
        finish,
        out_shape=(
            jax.ShapeDtypeStruct((COLS, ROWS), BF16),
            jax.ShapeDtypeStruct((ROWS, 128), BF16),
            jax.ShapeDtypeStruct((2, COLS, ROWS), F32),
        ),
        in_specs=[pl.BlockSpec(memory_space=pltpu.VMEM)] * 4,
        out_specs=[pl.BlockSpec(memory_space=pltpu.HBM)] * 3,
        scratch_shapes=[pltpu.VMEM((2, COLS, ROWS), F32), dma((4,))],
        compiler_params=pltpu.CompilerParams(vmem_limit_bytes=8 * 1024 * 1024),
    )(*made)
    return hidden.T, input_grad, update.transpose(0, 2, 1)


def solution(mesh):
    finer = Mesh(
        mesh.devices.reshape(4, 8, 2, 4, 2), ("outer_0", "outer_1", "inner_0", "inner_1", "inner_2")
    )
    return jax.shard_map(
        local,
        mesh=finer,
        in_specs=(
            P(INNER, None),
            P(None, INNER, OUTER),
            P(None, INNER, OUTER),
            P(None, INNER, OUTER),
            P(None, INNER, OUTER),
            P(INNER, OUTER),
        ),
        out_specs=(P(INNER, OUTER), P(INNER, OUTER), P(None, INNER, OUTER)),
        check_vma=False,
    )
```
